128 devices in a mesh: kpt: 1, col: 64 (over z, y, x), row: 2 (over core).
Axes of the slice: x: 4, y: 4, z: 4, core: 2. Of those that a mesh axis runs over, the one named last changes fastest.
Arguments:
- z_in: float32 [6144, 4096], P('kpt', ('col', 'row'))
- v_panels: float32 [6144, 6144], P(('kpt', 'row'), 'col')
- t_factors: float32 [192, 32, 32], P('kpt')
Outputs:
- output: float32 [6144, 4096], P(('kpt', 'row'), 'col')
All inputs are finite; a program needn't handle non-finite values.
Results may differ from the reference program's by a relative error of at most 0.001.
Values sent between devices are 32-bit elements.
A program may use at most 1 GiB of HBM per device.

```python
import jax
import jax.numpy as jnp
from jax import lax

N = 6144
BLK = 32
M = 4096
ROWS = 2
COLS = 64

PANELS = N // BLK
PRECISE = lax.Precision.HIGHEST


def setup_inputs(seed: int = 0, part: int = 0) -> dict:
    base_key = jax.random.fold_in(jax.random.key(seed), part)
    key_v, key_tau, key_z = jax.random.split(base_key, 3)
    row_ids = jnp.arange(N)[:, None]

    def build_panel(panel_idx):
        col_ids = panel_idx * BLK + jnp.arange(BLK)
        noise = jax.random.normal(jax.random.fold_in(key_v, panel_idx), (N, BLK), jnp.float32)
        spread = jax.random.uniform(jax.random.fold_in(key_tau, panel_idx), (BLK,), jnp.float32, 0.25, 3.0)
        tail_len = jnp.maximum(N - 1 - col_ids, 1).astype(jnp.float32)
        scale = jnp.sqrt(spread / tail_len)
        panel = jnp.where(row_ids > col_ids, noise * scale, (row_ids == col_ids).astype(jnp.float32))
        gram_mat = jnp.dot(panel.T, panel, precision=PRECISE, preferred_element_type=jnp.float32)
        t_inverse = jnp.triu(gram_mat, 1) + 0.5 * jnp.diag(jnp.diag(gram_mat))
        t_mat = jnp.triu(jnp.linalg.inv(t_inverse))
        return panel, t_mat

    panels, t_factors = lax.map(build_panel, jnp.arange(PANELS))
    v_panels = panels.reshape(PANELS // COLS, COLS, PANELS // ROWS, ROWS, BLK, BLK)
    v_panels = v_panels.transpose(3, 2, 4, 1, 0, 5).reshape(N, N)
    z_in = jax.random.normal(key_z, (N, M), jnp.float32)
    return {"z_in": z_in, "v_panels": v_panels, "t_factors": t_factors}


def reference(z_in, v_panels, t_factors):
    panels = v_panels.reshape(N, COLS, PANELS // COLS, BLK).transpose(2, 1, 0, 3).reshape(PANELS, N, BLK)

    def apply_panel(z_cur, panel_pair):
        panel, t_mat = panel_pair
        s_part = jnp.dot(panel.T, z_cur, precision=PRECISE, preferred_element_type=jnp.float32)
        w_part = jnp.dot(t_mat, s_part, precision=PRECISE, preferred_element_type=jnp.float32)
        z_next = z_cur - jnp.dot(panel, w_part, precision=PRECISE, preferred_element_type=jnp.float32)
        return z_next, None

    z_out, _ = lax.scan(apply_panel, z_in, (panels, t_factors), reverse=True)
    return z_out
```

```python
import jax
import jax.numpy as jnp
from jax import lax
from jax.experimental import pallas as pl
from jax.experimental.pallas import tpu as pltpu
from jax.sharding import PartitionSpec as P

PRECISE = lax.Precision.HIGHEST
MESH = pl.DeviceIdType.MESH

SIDE = 4
BLK = 32
ROUNDS = 3
LANES = 128
CHUNKS = 24
GROUP = 256
STEPS = 24
COLS = 64

ORDER = (("x", "y", "z"), ("y", "z", "x"), ("z", "x", "y"))
SHARES = {
    24: (8, 8, 8), 22: (8, 7, 7), 20: (7, 7, 6), 18: (6, 6, 6),
    16: (5, 5, 6), 14: (5, 5, 4), 12: (4, 4, 4), 10: (3, 3, 4),
    8: (3, 3, 2), 6: (2, 2, 2), 4: (1, 1, 2), 2: (1, 1, 0),
}
ROUND_BASE = (0, 24, 40)
SLOTS = 48
KINDS = ("A+", "A-", "F+", "F-")


def part(rnd, z_src, colour):
    first = 8 * rnd + 2 * z_src
    shares = SHARES[CHUNKS - first]
    return ROUND_BASE[rnd] + first - 8 * rnd + sum(shares[:colour]), shares[colour]


def sem_table():
    table = {}
    for rnd in range(ROUNDS):
        for colour in range(3):
            for phase in range(3):
                planes = range(SIDE) if "z" in ORDER[colour][:phase] else (None,)
                for kind in KINDS:
                    for plane in planes:
                        table[rnd, colour, phase, kind, plane] = len(table)
    return table


SEMS = sem_table()


class Gather:
    def __init__(self, buf, send_sems, recv_sems):
        col = lax.axis_index("col")
        self.kpt, self.core = lax.axis_index("kpt"), lax.axis_index("row")
        self.me = {"z": col // 16, "y": (col // 4) % 4, "x": col % 4}
        self.buf, self.send_sems, self.recv_sems = buf, send_sems, recv_sems
        self.at = {(axis, offset): (self.me[axis] + offset) % SIDE for axis in "xyz" for offset in (1, 2, 3)}
        self.peer = {(axis, offset): self.find(axis, offset) for axis in "xyz" for offset in (1, 3)}

    def find(self, axis, offset):
        at = dict(self.me)
        at[axis] = self.at[axis, offset]
        return (self.kpt, at["z"] * 16 + at["y"] * 4 + at["x"], self.core)

    def shifted(self, axis, offset):
        return self.me[axis] if offset == 0 else self.at[axis, offset % SIDE]

    def neighbour(self, axis, offset):
        return self.peer[axis, offset % SIDE]

    def each(self, rnd, colour, phase, kind, source, fn):
        axis = ORDER[colour][phase]
        whole = ORDER[colour][:phase]
        rows = {"A+": pl.ds(0, BLK), "A-": pl.ds(0, BLK), "F+": pl.ds(0, BLK // 2), "F-": pl.ds(BLK // 2, BLK // 2)}[kind]
        target = self.neighbour(axis, 1 if kind[1] == "+" else -1)

        def descriptor(plane, sem):
            slot, count = part(rnd, plane, colour)
            if count == 0:
                return
            at = {}
            for name in "zyx":
                if name in whole:
                    at[name] = slice(None)
                else:
                    at[name] = self.shifted(name, source) if name == axis else self.me[name]
            block = self.buf.at[pl.ds(slot, count), plane, at["y"], at["x"], rows, :]
            fn(
                pltpu.make_async_remote_copy(
                    src_ref=block, dst_ref=block,
                    send_sem=self.send_sems.at[sem], recv_sem=self.recv_sems.at[sem],
                    device_id=target, device_id_type=MESH,
                )
            )

        if "z" in whole:
            for plane in reversed(range(SIDE)):
                descriptor(plane, SEMS[rnd, colour, phase, kind, plane])
            return
        plane_here = self.shifted("z", source) if axis == "z" else self.me["z"]
        for plane in range(SIDE):
            pl.when(plane_here == plane)(
                lambda plane=plane: descriptor(plane, SEMS[rnd, colour, phase, kind, None])
            )

    def start_own(self, rnd, colour, phase):
        for kind in ("A+", "A-"):
            self.each(rnd, colour, phase, kind, 0, lambda copy: copy.start())

    def forward(self, rnd, colour, phase):
        for kind, relay, source in (("A+", "F+", -1), ("A-", "F-", 1)):
            self.each(rnd, colour, phase, kind, source, lambda copy: copy.wait_recv())
            self.each(rnd, colour, phase, relay, source, lambda copy: copy.start())

    def finish(self, rnd, colour, phase):
        for kind, source in (("F+", -2), ("F-", 2)):
            self.each(rnd, colour, phase, kind, source, lambda copy: copy.wait_recv())

    def event(self, name, rnd):
        for colour in range(3):
            if name == "A1":
                self.start_own(rnd, colour, 0)
            elif name in ("F1", "F2", "F3"):
                self.forward(rnd, colour, int(name[1]) - 1)
            elif name in ("A2", "A3"):
                self.finish(rnd, colour, int(name[1]) - 2)
                self.start_own(rnd, colour, int(name[1]) - 1)
            else:
                self.finish(rnd, colour, 2)

    def drain(self):
        for rnd in range(ROUNDS):
            for colour in range(3):
                for phase in range(3):
                    for kind, source in (("A+", 0), ("A-", 0), ("F+", -1), ("F-", 1)):
                        self.each(rnd, colour, phase, kind, source, lambda copy: copy.wait_send())


EVENTS = (
    ("A1", 2), ("A1", 1), ("A1", 0), ("F1", 2), ("A2", 2), ("F1", 1), ("F2", 2), ("A3", 2),
    ("A2", 1), ("F1", 0), ("F3", 2), ("F2", 1), ("A2", 0), ("A3", 1), ("F2", 0), ("F3", 1),
    ("A3", 0), ("D", 2), ("D", 1), ("F3", 0), ("D", 0),
)


def nt(lhs, rhs):
    return lax.dot_general(lhs, rhs, (((1,), (1,)), ((), ())), precision=PRECISE, preferred_element_type=jnp.float32)


def nn(lhs, rhs):
    return lax.dot_general(lhs, rhs, (((1,), (0,)), ((), ())), precision=PRECISE, preferred_element_type=jnp.float32)


def enter(gather, partner):
    barrier = pltpu.get_barrier_semaphore()
    peers = [] if gather is None else [gather.neighbour(axis, offset) for axis in "xyz" for offset in (1, -1)]
    for peer in peers + ([] if partner is None else [partner]):
        pl.semaphore_signal(barrier, inc=1, device_id=peer, device_id_type=MESH)
    pl.semaphore_wait(barrier, len(peers) + (partner is not None))


def gather_kernel(v_ref, out_ref, buf, send_sems, recv_sems, own_sems):
    gather = Gather(buf, send_sems, recv_sems)
    me = gather.me
    own = []
    for rnd in range(ROUNDS):
        copy = pltpu.make_async_copy(
            v_ref.at[rnd, pl.ds(8 * rnd, CHUNKS - 8 * rnd)],
            buf.at[pl.ds(ROUND_BASE[rnd], CHUNKS - 8 * rnd), me["z"], me["y"], me["x"]],
            own_sems.at[rnd],
        )
        copy.start()
        own.append(copy)
    enter(gather, None)
    for copy in own:
        copy.wait()
    for name, rnd in EVENTS:
        gather.event(name, rnd)
    gather.drain()
    whole = pltpu.make_async_copy(buf, out_ref, own_sems.at[0])
    whole.start()
    whole.wait()


def apply_kernel(z_ref, v_ref, t_ref, out_ref, buf, acc, peer, t_buf, v_sems, peer_send, peer_recv, t_sems):
    partner = (lax.axis_index("kpt"), lax.axis_index("col"), 1 - lax.axis_index("row"))

    def v_copy(rnd):
        block = pl.ds(ROUND_BASE[rnd], CHUNKS - 8 * rnd)
        return pltpu.make_async_copy(v_ref.at[block], buf.at[block], v_sems.at[rnd])

    for rnd in reversed(range(ROUNDS)):
        v_copy(rnd).start()
    enter(None, partner)
    out_ref[...] = z_ref[...]

    row = lax.broadcasted_iota(jnp.int32, (GROUP, GROUP), 0)
    column = lax.broadcasted_iota(jnp.int32, (GROUP, GROUP), 1)

    def t_copy(group, slot):
        return pltpu.make_async_copy(t_ref.at[group], t_buf.at[slot], t_sems.at[slot])

    t_copy(STEPS - 1, 0).start()

    def step(idx, _):
        for rnd_needed in range(ROUNDS):
            pl.when(idx == 16 - 8 * rnd_needed)(lambda rnd_needed=rnd_needed: v_copy(rnd_needed).wait())

        group = STEPS - 1 - idx
        rnd = group // 8
        plane = (group % 8) // 2
        pair = (group % 2) * 2
        slot = idx % 2
        shift = 16 * rnd - 4 * rnd * (rnd - 1)
        first = 4 * rnd + plane

        def tile(w):
            halves = [
                buf[shift + 2 * w + half, plane, pl.ds(pair, 2), :, :, :].reshape(GROUP, LANES) for half in range(2)
            ]
            return jnp.concatenate(halves, axis=1)

        def z_tile(w):
            return jnp.concatenate([out_ref[2 * w], out_ref[2 * w + 1]], axis=1)

        acc[...] = jnp.zeros_like(acc)

        def gram(w, _):
            v = tile(w)
            acc[...] += nt(jnp.concatenate([z_tile(w), v], axis=0), v)
            return 0

        lax.fori_loop(first, CHUNKS // 2, gram, 0)

        exchange = pltpu.make_async_remote_copy(
            src_ref=acc, dst_ref=peer.at[slot], send_sem=peer_send.at[slot], recv_sem=peer_recv.at[slot],
            device_id=partner, device_id_type=MESH,
        )
        exchange.start()

        @pl.when(idx < STEPS - 1)
        def _():
            t_copy(group - 1, 1 - slot).start()

        t_copy(group, slot).wait()
        exchange.wait()

        s_full = acc[pl.ds(0, COLS), :] + peer[slot, pl.ds(0, COLS), :]
        g_full = acc[pl.ds(COLS, GROUP), :] + peer[slot, pl.ds(COLS, GROUP), :]
        t_mat = t_buf[slot]
        for width in (BLK, 2 * BLK, 4 * BLK):
            mask = (row // (2 * width) == column // (2 * width)) & (row // width < column // width)
            t_mat = t_mat - nn(nn(t_mat, jnp.where(mask, g_full, 0.0)), t_mat)
        w_full = nt(s_full, t_mat)

        def update(w, _):
            delta = nn(w_full, tile(w))
            out_ref[2 * w] -= delta[:, :LANES]
            out_ref[2 * w + 1] -= delta[:, LANES:]
            return 0

        lax.fori_loop(first, CHUNKS // 2, update, 0)
        return 0

    lax.fori_loop(0, STEPS, step, 0)


def gather_panels(v):
    return pl.pallas_call(
        gather_kernel,
        out_shape=jax.ShapeDtypeStruct((SLOTS, SIDE, SIDE, SIDE, BLK, LANES), jnp.float32),
        in_specs=[pl.BlockSpec(memory_space=pl.ANY)],
        out_specs=pl.BlockSpec(memory_space=pl.ANY),
        scratch_shapes=[
            pltpu.VMEM((SLOTS, SIDE, SIDE, SIDE, BLK, LANES), jnp.float32),
            pltpu.SemaphoreType.DMA((len(SEMS),)),
            pltpu.SemaphoreType.DMA((len(SEMS),)),
            pltpu.SemaphoreType.DMA((ROUNDS,)),
        ],
        compiler_params=pltpu.CompilerParams(collective_id=0, has_side_effects=True, vmem_limit_bytes=60 * 1024 * 1024),
        name="gather_panels",
    )(v)


def apply_panels(z, v, t):
    return pl.pallas_call(
        apply_kernel,
        out_shape=jax.ShapeDtypeStruct(z.shape, jnp.float32),
        in_specs=[
            pl.BlockSpec(memory_space=pltpu.VMEM),
            pl.BlockSpec(memory_space=pl.ANY),
            pl.BlockSpec(memory_space=pl.ANY),
        ],
        out_specs=pl.BlockSpec(memory_space=pltpu.VMEM),
        scratch_shapes=[
            pltpu.VMEM((SLOTS, SIDE, SIDE, SIDE, BLK, LANES), jnp.float32),
            pltpu.VMEM((COLS + GROUP, GROUP), jnp.float32),
            pltpu.VMEM((2, COLS + GROUP, GROUP), jnp.float32),
            pltpu.VMEM((2, GROUP, GROUP), jnp.float32),
            pltpu.SemaphoreType.DMA((ROUNDS,)),
            pltpu.SemaphoreType.DMA((2,)),
            pltpu.SemaphoreType.DMA((2,)),
            pltpu.SemaphoreType.DMA((2,)),
        ],
        compiler_params=pltpu.CompilerParams(collective_id=1, has_side_effects=True, vmem_limit_bytes=60 * 1024 * 1024),
        name="apply_panels",
    )(z, v, t)


def solution(mesh):
    def local_run(z_cols, v_local, t_local):
        z = lax.all_to_all(z_cols, "row", 0, 1, tiled=True)
        z = z.reshape(CHUNKS, LANES, COLS).transpose(0, 2, 1)
        v = v_local.reshape(CHUNKS, LANES, ROUNDS, BLK).transpose(2, 0, 3, 1)
        blocks = GROUP // BLK
        same = jnp.eye(blocks, dtype=bool)[None, :, None, :, None]
        t = jnp.where(same, t_local.reshape(STEPS, blocks, BLK, 1, BLK), 0.0).reshape(STEPS, GROUP, GROUP)
        out = apply_panels(z, gather_panels(v), t)
        return out.transpose(0, 2, 1).reshape(CHUNKS * LANES, COLS)

    return jax.shard_map(
        local_run,
        mesh=mesh,
        in_specs=(P("kpt", ("col", "row")), P(("kpt", "row"), "col"), P("kpt", None, None)),
        out_specs=P(("kpt", "row"), "col"),
        check_vma=False,
    )
```

```python
import jax
import jax.numpy as jnp
from jax import lax
from jax.experimental import pallas as pl
from jax.experimental.pallas import tpu as pltpu
from jax.sharding import PartitionSpec as P

PRECISE = lax.Precision.HIGHEST
MESH = pl.DeviceIdType.MESH

SIDE = 4
BLK = 32
ROUNDS = 3
LANES = 128
CHUNKS = 24
GROUP = 256
STEPS = 24
COLS = 64

ORDER = (("x", "y", "z"), ("y", "z", "x"), ("z", "x", "y"))
SHARES = {
    24: (8, 8, 8), 22: (8, 7, 7), 20: (7, 7, 6), 18: (6, 6, 6),
    16: (5, 5, 6), 14: (5, 5, 4), 12: (4, 4, 4), 10: (3, 3, 4),
    8: (3, 3, 2), 6: (2, 2, 2), 4: (1, 1, 2), 2: (1, 1, 0),
}
ROUND_BASE = (0, 24, 40)
SLOTS = 48
KINDS = ("A+", "A-", "F+", "F-")


def part(rnd, z_src, colour):
    first = 8 * rnd + 2 * z_src
    shares = SHARES[CHUNKS - first]
    return ROUND_BASE[rnd] + first - 8 * rnd + sum(shares[:colour]), shares[colour]


def sem_table():
    table = {}
    for rnd in range(ROUNDS):
        for colour in range(3):
            for phase in range(3):
                planes = range(SIDE) if "z" in ORDER[colour][:phase] else (None,)
                for kind in KINDS:
                    for plane in planes:
                        table[rnd, colour, phase, kind, plane] = len(table)
    return table


SEMS = sem_table()


class Gather:
    def __init__(self, buf, send_sems, recv_sems):
        col = lax.axis_index("col")
        self.kpt, self.core = lax.axis_index("kpt"), lax.axis_index("row")
        self.me = {"z": col // 16, "y": (col // 4) % 4, "x": col % 4}
        self.buf, self.send_sems, self.recv_sems = buf, send_sems, recv_sems
        self.at = {(axis, offset): (self.me[axis] + offset) % SIDE for axis in "xyz" for offset in (1, 2, 3)}
        self.peer = {(axis, offset): self.find(axis, offset) for axis in "xyz" for offset in (1, 3)}

    def find(self, axis, offset):
        at = dict(self.me)
        at[axis] = self.at[axis, offset]
        return (self.kpt, at["z"] * 16 + at["y"] * 4 + at["x"], self.core)

    def shifted(self, axis, offset):
        return self.me[axis] if offset == 0 else self.at[axis, offset % SIDE]

    def neighbour(self, axis, offset):
        return self.peer[axis, offset % SIDE]

    def each(self, rnd, colour, phase, kind, source, fn):
        axis = ORDER[colour][phase]
        whole = ORDER[colour][:phase]
        rows = {"A+": pl.ds(0, BLK), "A-": pl.ds(0, BLK), "F+": pl.ds(0, BLK // 2), "F-": pl.ds(BLK // 2, BLK // 2)}[kind]
        target = self.neighbour(axis, 1 if kind[1] == "+" else -1)

        def descriptor(plane, sem):
            slot, count = part(rnd, plane, colour)
            if count == 0:
                return
            at = {}
            for name in "zyx":
                if name in whole:
                    at[name] = slice(None)
                else:
                    at[name] = self.shifted(name, source) if name == axis else self.me[name]
            block = self.buf.at[pl.ds(slot, count), plane, at["y"], at["x"], rows, :]
            fn(
                pltpu.make_async_remote_copy(
                    src_ref=block, dst_ref=block,
                    send_sem=self.send_sems.at[sem], recv_sem=self.recv_sems.at[sem],
                    device_id=target, device_id_type=MESH,
                )
            )

        if "z" in whole:
            for plane in reversed(range(SIDE)):
                descriptor(plane, SEMS[rnd, colour, phase, kind, plane])
            return
        plane_here = self.shifted("z", source) if axis == "z" else self.me["z"]
        for plane in range(SIDE):
            pl.when(plane_here == plane)(
                lambda plane=plane: descriptor(plane, SEMS[rnd, colour, phase, kind, None])
            )

    def start_own(self, rnd, colour, phase):
        for kind in ("A+", "A-"):
            self.each(rnd, colour, phase, kind, 0, lambda copy: copy.start())

    def forward(self, rnd, colour, phase):
        for kind, relay, source in (("A+", "F+", -1), ("A-", "F-", 1)):
            self.each(rnd, colour, phase, kind, source, lambda copy: copy.wait_recv())
            self.each(rnd, colour, phase, relay, source, lambda copy: copy.start())

    def finish(self, rnd, colour, phase):
        for kind, source in (("F+", -2), ("F-", 2)):
            self.each(rnd, colour, phase, kind, source, lambda copy: copy.wait_recv())

    def event(self, name, rnd, colours):
        for colour in colours:
            if name == "A1":
                self.start_own(rnd, colour, 0)
            elif name in ("F1", "F2", "F3"):
                self.forward(rnd, colour, int(name[1]) - 1)
            elif name in ("A2", "A3"):
                self.finish(rnd, colour, int(name[1]) - 2)
                self.start_own(rnd, colour, int(name[1]) - 1)
            else:
                self.finish(rnd, colour, 2)

    def drain(self):
        for rnd in range(ROUNDS):
            for colour in range(3):
                for phase in range(3):
                    for kind, source in (("A+", 0), ("A-", 0), ("F+", -1), ("F-", 1)):
                        self.each(rnd, colour, phase, kind, source, lambda copy: copy.wait_send())


ALL = (0, 1, 2)
OPENING = (
    ("A1", 2, ALL), ("A1", 1, ALL), ("A1", 0, ALL), ("F1", 2, ALL), ("A2", 2, ALL), ("F2", 2, ALL), ("A3", 2, ALL),
    ("F1", 1, ALL), ("A2", 1, ALL), ("F1", 0, ALL), ("F3", 2, ALL), ("F2", 1, ALL), ("A3", 1, ALL), ("A2", 0, ALL),
    ("D", 2, ALL),
)
BEFORE_STEP = {
    1: (("F2", 0, ALL),), 3: (("F3", 1, ALL),), 4: (("A3", 0, ALL),), 8: (("D", 1, ALL),), 12: (("F3", 0, ALL),),
    16: (("D", 0, ALL),),
}


def nt(lhs, rhs):
    return lax.dot_general(lhs, rhs, (((1,), (1,)), ((), ())), precision=PRECISE, preferred_element_type=jnp.float32)


def nn(lhs, rhs):
    return lax.dot_general(lhs, rhs, (((1,), (0,)), ((), ())), precision=PRECISE, preferred_element_type=jnp.float32)


def kernel(
    z_ref, v_ref, t_ref, out_ref, buf, acc, peer, t_buf,
    send_sems, recv_sems, own_sems, z_sems, peer_send, peer_recv, t_sems,
):
    gather = Gather(buf, send_sems, recv_sems)
    me, core = gather.me, gather.core
    partner = (gather.kpt, lax.axis_index("col"), 1 - core)

    own = []
    for rnd in reversed(range(ROUNDS)):
        copy = pltpu.make_async_copy(
            v_ref.at[rnd, pl.ds(8 * rnd, CHUNKS - 8 * rnd)],
            buf.at[pl.ds(ROUND_BASE[rnd], CHUNKS - 8 * rnd), me["z"], me["y"], me["x"]],
            own_sems.at[rnd],
        )
        copy.start()
        own.append(copy)
    mine = pl.ds(core * (COLS // 2), COLS // 2)
    z_keep = pltpu.make_async_copy(z_ref.at[core], out_ref.at[:, mine, :], z_sems.at[0])
    z_keep.start()

    barrier = pltpu.get_barrier_semaphore()
    for axis in "xyz":
        for offset in (1, -1):
            pl.semaphore_signal(barrier, inc=1, device_id=gather.neighbour(axis, offset), device_id_type=MESH)
    pl.semaphore_signal(barrier, inc=1, device_id=partner, device_id_type=MESH)
    pl.semaphore_wait(barrier, 7)

    for copy in own:
        copy.wait()
    for event in OPENING[:3]:
        gather.event(*event)
    z_give = pltpu.make_async_remote_copy(
        src_ref=z_ref.at[1 - core], dst_ref=out_ref.at[:, mine, :], send_sem=z_sems.at[1], recv_sem=z_sems.at[2],
        device_id=partner, device_id_type=MESH,
    )
    z_give.start()
    for event in OPENING[3:]:
        gather.event(*event)
    z_keep.wait()
    z_give.wait()

    row = lax.broadcasted_iota(jnp.int32, (GROUP, GROUP), 0)
    column = lax.broadcasted_iota(jnp.int32, (GROUP, GROUP), 1)

    def t_copy(group, slot):
        return pltpu.make_async_copy(t_ref.at[group], t_buf.at[slot], t_sems.at[slot])

    t_copy(STEPS - 1, 0).start()

    def step(idx, _):
        for at, events in BEFORE_STEP.items():
            @pl.when(idx == at)
            def _(events=events):
                for event in events:
                    gather.event(*event)

        group = STEPS - 1 - idx
        rnd = group // 8
        plane = (group % 8) // 2
        pair = (group % 2) * 2
        slot = idx % 2
        shift = 16 * rnd - 4 * rnd * (rnd - 1)
        first = 4 * rnd + plane

        def tile(w):
            halves = [
                buf[shift + 2 * w + half, plane, pl.ds(pair, 2), :, :, :].reshape(GROUP, LANES) for half in range(2)
            ]
            return jnp.concatenate(halves, axis=1)

        def z_tile(w):
            return jnp.concatenate([out_ref[2 * w], out_ref[2 * w + 1]], axis=1)

        acc[...] = jnp.zeros_like(acc)

        def gram(w, _):
            v = tile(w)
            acc[...] += nt(jnp.concatenate([z_tile(w), v], axis=0), v)
            return 0

        lax.fori_loop(first, CHUNKS // 2, gram, 0)

        exchange = pltpu.make_async_remote_copy(
            src_ref=acc, dst_ref=peer.at[slot], send_sem=peer_send.at[slot], recv_sem=peer_recv.at[slot],
            device_id=partner, device_id_type=MESH,
        )
        exchange.start()

        @pl.when(idx < STEPS - 1)
        def _():
            t_copy(group - 1, 1 - slot).start()

        t_copy(group, slot).wait()
        exchange.wait()

        s_full = acc[pl.ds(0, COLS), :] + peer[slot, pl.ds(0, COLS), :]
        g_full = acc[pl.ds(COLS, GROUP), :] + peer[slot, pl.ds(COLS, GROUP), :]
        compact = t_buf[slot]
        t_mat = jnp.where(
            row // BLK == column // BLK, jnp.concatenate([compact] * (GROUP // BLK), axis=1), 0.0
        )
        for width in (BLK, 2 * BLK, 4 * BLK):
            mask = (row // (2 * width) == column // (2 * width)) & (row // width < column // width)
            t_mat = t_mat - nn(nn(t_mat, jnp.where(mask, g_full, 0.0)), t_mat)
        w_full = nt(s_full, t_mat)

        def update(w, _):
            delta = nn(w_full, tile(w))
            out_ref[2 * w] -= delta[:, :LANES]
            out_ref[2 * w + 1] -= delta[:, LANES:]
            return 0

        lax.fori_loop(first, CHUNKS // 2, update, 0)
        return 0

    lax.fori_loop(0, STEPS, step, 0)
    gather.drain()


def apply_panels(z, v, t):
    return pl.pallas_call(
        kernel,
        out_shape=jax.ShapeDtypeStruct((CHUNKS, COLS, LANES), jnp.float32),
        in_specs=[pl.BlockSpec(memory_space=pl.ANY)] * 3,
        out_specs=pl.BlockSpec(memory_space=pltpu.VMEM),
        scratch_shapes=[
            pltpu.VMEM((SLOTS, SIDE, SIDE, SIDE, BLK, LANES), jnp.float32),
            pltpu.VMEM((COLS + GROUP, GROUP), jnp.float32),
            pltpu.VMEM((2, COLS + GROUP, GROUP), jnp.float32),
            pltpu.VMEM((2, GROUP, BLK), jnp.float32),
            pltpu.SemaphoreType.DMA((len(SEMS),)),
            pltpu.SemaphoreType.DMA((len(SEMS),)),
            pltpu.SemaphoreType.DMA((ROUNDS,)),
            pltpu.SemaphoreType.DMA((3,)),
            pltpu.SemaphoreType.DMA((2,)),
            pltpu.SemaphoreType.DMA((2,)),
            pltpu.SemaphoreType.DMA((2,)),
        ],
        compiler_params=pltpu.CompilerParams(collective_id=0, has_side_effects=True, vmem_limit_bytes=60 * 1024 * 1024),
        name="apply_panels",
    )(z, v, t)


def solution(mesh):
    def local_run(z_cols, v_local, t_local):
        z = z_cols.reshape(2, CHUNKS, LANES, COLS // 2).transpose(0, 1, 3, 2)
        v = v_local.reshape(CHUNKS, LANES, ROUNDS, BLK).transpose(2, 0, 3, 1)
        out = apply_panels(z, v, t_local.reshape(STEPS, GROUP, BLK))
        return out.transpose(0, 2, 1).reshape(CHUNKS * LANES, COLS)

    return jax.shard_map(
        local_run,
        mesh=mesh,
        in_specs=(P("kpt", ("col", "row")), P(("kpt", "row"), "col"), P("kpt", None, None)),
        out_specs=P(("kpt", "row"), "col"),
        check_vma=False,
    )
```

```python
import jax
import jax.numpy as jnp
from jax import lax
from jax.experimental import pallas as pl
from jax.experimental.pallas import tpu as pltpu
from jax.sharding import PartitionSpec as P

PRECISE = lax.Precision.HIGHEST
MESH = pl.DeviceIdType.MESH

SIDE = 4
BLK = 32
ROUNDS = 3
LANES = 128
CHUNKS = 24
GROUP = 256
STEPS = 24
COLS = 64

ORDER = (("x", "y", "z"), ("y", "z", "x"), ("z", "x", "y"))
SHARES = {
    24: (8, 8, 8), 22: (8, 7, 7), 20: (7, 7, 6), 18: (6, 6, 6),
    16: (5, 5, 6), 14: (5, 5, 4), 12: (4, 4, 4), 10: (3, 3, 4),
    8: (3, 3, 2), 6: (2, 2, 2), 4: (1, 1, 2), 2: (1, 1, 0),
}
ROUND_BASE = (0, 24, 40)
SLOTS = 48
KINDS = ("A+", "A-", "F+", "F-")
FACTOR = 3
OCTET = 8
SHARE = 16


def axes_of(rnd, colour):
    return ORDER[rnd if colour == FACTOR else colour]


def part(rnd, z_src, colour):
    first = 8 * rnd + 2 * z_src
    shares = SHARES[CHUNKS - first]
    return ROUND_BASE[rnd] + first - 8 * rnd + sum(shares[:colour]), shares[colour]


def sem_table():
    table = {}
    for rnd in range(ROUNDS):
        for colour in range(4):
            for phase in range(3):
                planes = range(SIDE) if colour != FACTOR and "z" in ORDER[colour][:phase] else (None,)
                for kind in KINDS:
                    for plane in planes:
                        table[rnd, colour, phase, kind, plane] = len(table)
    return table


SEMS = sem_table()


class Gather:
    def __init__(self, buf, factors, send_sems, recv_sems):
        col = lax.axis_index("col")
        self.kpt, self.core = lax.axis_index("kpt"), lax.axis_index("row")
        self.me = {"z": col // 16, "y": (col // 4) % 4, "x": col % 4}
        self.buf, self.factors, self.send_sems, self.recv_sems = buf, factors, send_sems, recv_sems
        self.at = {(axis, offset): (self.me[axis] + offset) % SIDE for axis in "xyz" for offset in (1, 2, 3)}
        self.peer = {(axis, offset): self.find(axis, offset) for axis in "xyz" for offset in (1, 3)}

    def find(self, axis, offset):
        at = dict(self.me)
        at[axis] = self.at[axis, offset]
        return (self.kpt, at["z"] * 16 + at["y"] * 4 + at["x"], self.core)

    def shifted(self, axis, offset):
        return self.me[axis] if offset == 0 else self.at[axis, offset % SIDE]

    def neighbour(self, axis, offset):
        return self.peer[axis, offset % SIDE]

    def each(self, rnd, colour, phase, kind, source, fn, planes=None):
        axis = axes_of(rnd, colour)[phase]
        whole = axes_of(rnd, colour)[:phase]
        rows = {"A+": pl.ds(0, BLK), "A-": pl.ds(0, BLK), "F+": pl.ds(0, BLK // 2), "F-": pl.ds(BLK // 2, BLK // 2)}[kind]
        target = self.neighbour(axis, 1 if kind[1] == "+" else -1)

        def coordinate(name):
            if name in whole:
                return slice(None)
            return self.shifted(name, source) if name == axis else self.me[name]

        def send(block, sem):
            fn(
                pltpu.make_async_remote_copy(
                    src_ref=block, dst_ref=block,
                    send_sem=self.send_sems.at[sem], recv_sem=self.recv_sems.at[sem],
                    device_id=target, device_id_type=MESH,
                )
            )

        def panels(plane, sem):
            slot, count = part(rnd, plane, colour)
            if count:
                send(self.buf.at[pl.ds(slot, count), plane, coordinate("y"), coordinate("x"), rows, :], sem)

        if colour == FACTOR:
            block = self.factors.at[self.core, rnd, coordinate("z"), coordinate("y"), coordinate("x"), rows, :]
            send(block, SEMS[rnd, colour, phase, kind, None])
        elif "z" in whole:
            for plane in reversed(range(SIDE)) if planes is None else planes:
                panels(plane, SEMS[rnd, colour, phase, kind, plane])
        else:
            plane_here = self.shifted("z", source) if axis == "z" else self.me["z"]
            for plane in range(SIDE):
                pl.when(plane_here == plane)(
                    lambda plane=plane: panels(plane, SEMS[rnd, colour, phase, kind, None])
                )

    def start_own(self, rnd, colour, phase):
        for kind in ("A+", "A-"):
            self.each(rnd, colour, phase, kind, 0, lambda copy: copy.start())

    def forward(self, rnd, colour, phase, planes=None):
        for kind, relay, source in (("A+", "F+", -1), ("A-", "F-", 1)):
            self.each(rnd, colour, phase, kind, source, lambda copy: copy.wait_recv(), planes)
            self.each(rnd, colour, phase, relay, source, lambda copy: copy.start(), planes)

    def finish(self, rnd, colour, phase, planes=None):
        for kind, source in (("F+", -2), ("F-", 2)):
            self.each(rnd, colour, phase, kind, source, lambda copy: copy.wait_recv(), planes)

    def event(self, name, rnd, colours, planes=None):
        for colour in colours:
            if name == "A1":
                self.start_own(rnd, colour, 0)
            elif name in ("F1", "F2", "F3"):
                self.forward(rnd, colour, int(name[1]) - 1, planes)
            elif name in ("A2", "A3"):
                self.finish(rnd, colour, int(name[1]) - 2)
                self.start_own(rnd, colour, int(name[1]) - 1)
            else:
                self.finish(rnd, colour, 2, planes)

    def drain(self):
        for rnd in range(ROUNDS):
            for colour in range(4):
                for phase in range(3):
                    for kind, source in (("A+", 0), ("A-", 0), ("F+", -1), ("F-", 1)):
                        self.each(rnd, colour, phase, kind, source, lambda copy: copy.wait_send())


ALL = (0, 1, 2)
T = (FACTOR,)
AFTER_SPREAD = (("A1", 2, ALL), ("A1", 1, ALL))
AFTER_GRAM = (("F1", 2, ALL),)
AFTER_PAIR = (("A2", 2, ALL),)
AFTER_SUM = (("F2", 2, ALL), ("F1", 1, ALL))
AFTER_GRAMS = (("A3", 2, ALL), ("A1", 0, ALL), ("A2", 1, ALL))
AFTER_FACTORS = (
    ("A1", 2, T), ("A1", 1, T), ("A1", 0, T), ("F1", 2, T), ("F1", 1, T), ("F1", 0, T),
    ("A2", 2, T), ("A2", 1, T), ("A2", 0, T), ("F1", 0, ALL), ("F3", 2, ALL), ("F2", 1, ALL),
    ("F2", 2, T), ("F2", 1, T), ("F2", 0, T), ("A3", 2, T), ("A3", 1, T), ("A3", 0, T), ("A3", 1, ALL),
    ("A2", 0, ALL), ("F3", 2, T), ("F3", 1, T), ("F3", 0, T), ("D", 2, ALL), ("D", 2, T), ("D", 1, T), ("D", 0, T),
)
BEFORE_STEP = {
    2: (("F2", 0, ALL),), 5: (("F3", 1, ALL), ("A3", 0, ALL)), 8: (("D", 1, ALL),),
    14: (("F3", 0, ALL),), 16: (("D", 0, ALL),),
}


def nt(lhs, rhs):
    return lax.dot_general(lhs, rhs, (((1,), (1,)), ((), ())), precision=PRECISE, preferred_element_type=jnp.float32)


def nn(lhs, rhs):
    return lax.dot_general(lhs, rhs, (((1,), (0,)), ((), ())), precision=PRECISE, preferred_element_type=jnp.float32)


def merge_factors(t, grams):
    row = lax.broadcasted_iota(jnp.int32, (GROUP, GROUP), 0)
    column = lax.broadcasted_iota(jnp.int32, (GROUP, GROUP), 1)
    for width in (BLK, 2 * BLK, 4 * BLK):
        above = (row // (2 * width) == column // (2 * width)) & (row // width < column // width)
        left = [nn(t_mat, jnp.where(above, gram, 0.0)) for t_mat, gram in zip(t, grams)]
        t = [t_mat - nn(half, t_mat) for t_mat, half in zip(t, left)]
    return t


def kernel(
    z_ref, v_ref, octet_ref, t_ref, out_ref, buf, factors, acc, peer, t_buf, rows_buf, gram, gram_peer, gram_pair,
    gram_parts, gram_full,
    send_sems, recv_sems, own_sems, z_sems, peer_send, peer_recv, octet_send, octet_recv, pair_send, pair_recv,
):
    gather = Gather(buf, factors, send_sems, recv_sems)
    me, core = gather.me, gather.core
    col = lax.axis_index("col")
    partner = (gather.kpt, col, 1 - core)
    seat = col % OCTET
    mates = {hop: (seat + hop) % OCTET for hop in range(1, OCTET)}

    def mate(hop):
        return (gather.kpt, col - seat + mates[hop], core)

    def to_mate(stage, hop, source, target):
        sem = stage * OCTET + hop
        return pltpu.make_async_remote_copy(
            src_ref=source, dst_ref=target, send_sem=octet_send.at[sem], recv_sem=octet_recv.at[sem],
            device_id=mate(hop), device_id_type=MESH,
        )

    def to_partner(sem, source, target):
        return pltpu.make_async_remote_copy(
            src_ref=source, dst_ref=target, send_sem=pair_send.at[sem], recv_sem=pair_recv.at[sem],
            device_id=partner, device_id_type=MESH,
        )

    own = [
        pltpu.make_async_copy(v_ref, buf.at[:, me["z"], me["y"], me["x"]], own_sems.at[0]),
        pltpu.make_async_copy(octet_ref.at[:, seat], rows_buf.at[:, seat], own_sems.at[1]),
    ]
    for rnd in range(ROUNDS):
        own.append(pltpu.make_async_copy(t_ref.at[8 * rnd + col // OCTET], t_buf.at[rnd], own_sems.at[2 + rnd]))
    for copy in own:
        copy.start()
    mine = pl.ds(core * (COLS // 2), COLS // 2)
    z_keep = pltpu.make_async_copy(z_ref.at[core], out_ref.at[:, mine, :], z_sems.at[0])
    z_keep.start()

    barrier = pltpu.get_barrier_semaphore()
    peers = [gather.neighbour(axis, offset) for axis in "xyz" for offset in (1, -1)]
    peers += [mate(hop) for hop in mates] + [partner]
    for device in peers:
        pl.semaphore_signal(barrier, inc=1, device_id=device, device_id_type=MESH)
    pl.semaphore_wait(barrier, len(peers))

    def run(events):
        for event in events:
            gather.event(*event)

    spread = [to_mate(0, hop, octet_ref.at[:, at], rows_buf.at[:, seat]) for hop, at in mates.items()]
    for copy in spread:
        copy.start()
    for copy in own:
        copy.wait()
    run(AFTER_SPREAD)
    z_give = pltpu.make_async_remote_copy(
        src_ref=z_ref.at[1 - core], dst_ref=out_ref.at[:, mine, :], send_sem=z_sems.at[1], recv_sem=z_sems.at[2],
        device_id=partner, device_id_type=MESH,
    )
    z_give.start()
    for copy in spread:
        copy.wait()
    for rnd, chunks in enumerate(((0, 1, 2), (3, 4), (5,))):
        panel = jnp.concatenate([rows_buf[chunk].reshape(GROUP, LANES) for chunk in chunks], axis=1)
        gram[:, :, rnd] = nt(panel, panel).reshape(OCTET, 2, SHARE, GROUP)
    pair = to_partner(0, gram.at[:, 1 - core], gram_peer)
    pair.start()
    run(AFTER_GRAM)
    pair.wait()
    gram_pair[...] = gram[:, core] + gram_peer[...]
    scatter = [to_mate(1, hop, gram_pair.at[at], gram_parts.at[seat]) for hop, at in mates.items()]
    for copy in scatter:
        copy.start()
    gram_parts[seat] = gram_pair[seat]
    run(AFTER_PAIR)
    for copy in scatter:
        copy.wait()
    gram_full[core, seat] = jnp.sum(gram_parts[...], axis=0)
    collect = [to_mate(2, hop, gram_full.at[core, seat], gram_full.at[core, seat]) for hop in mates]
    for copy in collect:
        copy.start()
    run(AFTER_SUM)
    for copy in collect:
        copy.wait()
    pair = to_partner(1, gram_full.at[core], gram_full.at[core])
    pair.start()
    run(AFTER_GRAMS)
    pair.wait()

    row = lax.broadcasted_iota(jnp.int32, (GROUP, GROUP), 0)
    column = lax.broadcasted_iota(jnp.int32, (GROUP, GROUP), 1)
    blocks = [
        jnp.where(row // BLK == column // BLK, jnp.concatenate([t_buf[rnd]] * OCTET, axis=1), 0.0)
        for rnd in range(ROUNDS)
    ]
    grams = [
        jnp.concatenate([gram_full[half, at, rnd] for at in range(OCTET) for half in range(2)], axis=0)
        for rnd in range(ROUNDS)
    ]
    for rnd, t_mat in enumerate(merge_factors(blocks, grams)):
        for half in range(2):
            rows_buf[2 * rnd + half] = t_mat[:, half * LANES : (half + 1) * LANES].reshape(OCTET, BLK, LANES)
        factors[core, rnd, me["z"], me["y"], me["x"]] = rows_buf[2 * rnd + core, seat]
    run(AFTER_FACTORS)
    halves = [to_partner(2 + rnd, factors.at[core, rnd], factors.at[core, rnd]) for rnd in range(ROUNDS)]
    for copy in reversed(halves):
        copy.start()
    z_keep.wait()
    z_give.wait()
    for copy in halves:
        copy.wait()

    def step(idx, _):
        for at, events in BEFORE_STEP.items():
            @pl.when(idx == at)
            def _(events=events):
                for event in events:
                    gather.event(*event)

        group = STEPS - 1 - idx
        rnd = group // 8
        plane = (group % 8) // 2
        pair_row = (group % 2) * 2
        slot = idx % 2
        shift = 16 * rnd - 4 * rnd * (rnd - 1)
        first = 4 * rnd + plane

        def tile(w):
            halves = [
                buf[shift + 2 * w + half, plane, pl.ds(pair_row, 2), :, :, :].reshape(GROUP, LANES) for half in range(2)
            ]
            return jnp.concatenate(halves, axis=1)

        def z_tile(w):
            return jnp.concatenate([out_ref[2 * w], out_ref[2 * w + 1]], axis=1)

        acc[...] = jnp.zeros_like(acc)

        def project(w, _):
            acc[...] += nt(z_tile(w), tile(w))
            return 0

        lax.fori_loop(first, CHUNKS // 2, project, 0)

        exchange = pltpu.make_async_remote_copy(
            src_ref=acc, dst_ref=peer.at[slot], send_sem=peer_send.at[slot], recv_sem=peer_recv.at[slot],
            device_id=partner, device_id_type=MESH,
        )
        exchange.start()

        t_mat = jnp.concatenate(
            [factors[half, rnd, plane, pl.ds(pair_row, 2)].reshape(GROUP, LANES) for half in range(2)], axis=1
        )
        exchange.wait()
        w_full = nt(acc[...] + peer[slot], t_mat)

        def update(w, _):
            delta = nn(w_full, tile(w))
            out_ref[2 * w] -= delta[:, :LANES]
            out_ref[2 * w + 1] -= delta[:, LANES:]
            return 0

        lax.fori_loop(first, CHUNKS // 2, update, 0)
        return 0

    lax.fori_loop(0, STEPS, step, 0)
    gather.drain()


def apply_panels(z, v, t):
    def vmem(*shape):
        return pltpu.VMEM(shape, jnp.float32)

    return pl.pallas_call(
        kernel,
        out_shape=jax.ShapeDtypeStruct((CHUNKS, COLS, LANES), jnp.float32),
        in_specs=[pl.BlockSpec(memory_space=pl.ANY)] * 4,
        out_specs=pl.BlockSpec(memory_space=pltpu.VMEM),
        scratch_shapes=[
            vmem(SLOTS, SIDE, SIDE, SIDE, BLK, LANES),
            vmem(2, ROUNDS, SIDE, SIDE, SIDE, BLK, LANES),
            vmem(COLS, GROUP),
            vmem(2, COLS, GROUP),
            vmem(ROUNDS, GROUP, BLK),
            vmem(SLOTS // OCTET, OCTET, BLK, LANES),
            vmem(OCTET, 2, ROUNDS, SHARE, GROUP),
            vmem(OCTET, ROUNDS, SHARE, GROUP),
            vmem(OCTET, ROUNDS, SHARE, GROUP),
            vmem(OCTET, ROUNDS, SHARE, GROUP),
            vmem(2, OCTET, ROUNDS, SHARE, GROUP),
            pltpu.SemaphoreType.DMA((len(SEMS),)),
            pltpu.SemaphoreType.DMA((len(SEMS),)),
            pltpu.SemaphoreType.DMA((2 + ROUNDS,)),
            pltpu.SemaphoreType.DMA((3,)),
            pltpu.SemaphoreType.DMA((2,)),
            pltpu.SemaphoreType.DMA((2,)),
            pltpu.SemaphoreType.DMA((3 * OCTET,)),
            pltpu.SemaphoreType.DMA((3 * OCTET,)),
            pltpu.SemaphoreType.DMA((2 + ROUNDS,)),
            pltpu.SemaphoreType.DMA((2 + ROUNDS,)),
        ],
        compiler_params=pltpu.CompilerParams(collective_id=0, has_side_effects=True, vmem_limit_bytes=67043328),
        name="apply_panels",
    )(z, v, v.reshape(SLOTS // OCTET, OCTET, BLK, LANES), t)


def solution(mesh):
    def local_run(z_cols, v_local, t_local):
        z = z_cols.reshape(2, CHUNKS, LANES, COLS // 2).transpose(0, 1, 3, 2)
        v = v_local.reshape(CHUNKS, LANES, ROUNDS, BLK).transpose(2, 0, 3, 1)
        v = jnp.concatenate([v[rnd, 8 * rnd :] for rnd in range(ROUNDS)], axis=0)
        out = apply_panels(z, v, t_local.reshape(STEPS, GROUP, BLK))
        return out.transpose(0, 2, 1).reshape(CHUNKS * LANES, COLS)

    return jax.shard_map(
        local_run,
        mesh=mesh,
        in_specs=(P("kpt", ("col", "row")), P(("kpt", "row"), "col"), P("kpt", None, None)),
        out_specs=P(("kpt", "row"), "col"),
        check_vma=False,
    )
```

```python
import jax
import jax.numpy as jnp
from jax import lax
from jax.experimental import pallas as pl
from jax.experimental.pallas import tpu as pltpu
from jax.sharding import PartitionSpec as P

PRECISE = lax.Precision.HIGHEST
MESH = pl.DeviceIdType.MESH

SIDE = 4
BLK = 32
ROUNDS = 3
LANES = 128
CHUNKS = 24
GROUP = 256
STEPS = 24
COLS = 64

ORDER = (("x", "y", "z"), ("y", "z", "x"), ("z", "x", "y"))
SHARES = {
    24: (4, 10, 10), 22: (4, 9, 9), 20: (4, 8, 8), 18: (4, 7, 7),
    16: (6, 5, 5), 14: (4, 5, 5), 12: (4, 4, 4), 10: (4, 3, 3),
    8: (2, 3, 3), 6: (2, 2, 2), 4: (2, 1, 1), 2: (1, 0, 1),
}
ROWS_BASE = (0, 3, 5)
ROUND_BASE = (0, 24, 40)
SLOTS = 48
KINDS = ("A+", "A-", "F+", "F-")
FACTOR = 3
OCTET = 8
SHARE = 16


def axes_of(rnd, colour):
    return ORDER[rnd if colour == FACTOR else colour]


def part(rnd, z_src, colour):
    first = 8 * rnd + 2 * z_src
    shares = SHARES[CHUNKS - first]
    return ROUND_BASE[rnd] + first - 8 * rnd + sum(shares[:colour]), shares[colour]


def sem_table():
    table = {}
    for rnd in range(ROUNDS):
        for colour in range(4):
            for phase in range(3):
                planes = range(SIDE) if colour != FACTOR and "z" in ORDER[colour][:phase] else (None,)
                for kind in KINDS:
                    for plane in planes:
                        table[rnd, colour, phase, kind, plane] = len(table)
    return table


SEMS = sem_table()


class Gather:
    def __init__(self, buf, factors, send_sems, recv_sems):
        col = lax.axis_index("col")
        self.kpt, self.core = lax.axis_index("kpt"), lax.axis_index("row")
        self.me = {"z": col // 16, "y": (col // 4) % 4, "x": col % 4}
        self.buf, self.factors, self.send_sems, self.recv_sems = buf, factors, send_sems, recv_sems
        self.at = {(axis, offset): (self.me[axis] + offset) % SIDE for axis in "xyz" for offset in (1, 2, 3)}
        self.peer = {(axis, offset): self.find(axis, offset) for axis in "xyz" for offset in (1, 3)}

    def find(self, axis, offset):
        at = dict(self.me)
        at[axis] = self.at[axis, offset]
        return (self.kpt, at["z"] * 16 + at["y"] * 4 + at["x"], self.core)

    def shifted(self, axis, offset):
        return self.me[axis] if offset == 0 else self.at[axis, offset % SIDE]

    def neighbour(self, axis, offset):
        return self.peer[axis, offset % SIDE]

    def each(self, rnd, colour, phase, kind, source, fn, planes=None):
        axis = axes_of(rnd, colour)[phase]
        whole = axes_of(rnd, colour)[:phase]
        rows = {"A+": pl.ds(0, BLK), "A-": pl.ds(0, BLK), "F+": pl.ds(0, BLK // 2), "F-": pl.ds(BLK // 2, BLK // 2)}[kind]
        target = self.neighbour(axis, 1 if kind[1] == "+" else -1)

        def coordinate(name):
            if name in whole:
                return slice(None)
            return self.shifted(name, source) if name == axis else self.me[name]

        def send(block, sem):
            fn(
                pltpu.make_async_remote_copy(
                    src_ref=block, dst_ref=block,
                    send_sem=self.send_sems.at[sem], recv_sem=self.recv_sems.at[sem],
                    device_id=target, device_id_type=MESH,
                )
            )

        def panels(plane, sem):
            slot, count = part(rnd, plane, colour)
            if count:
                send(self.buf.at[pl.ds(slot, count), plane, coordinate("y"), coordinate("x"), rows, :], sem)

        if colour == FACTOR:
            block = self.factors.at[self.core, rnd, coordinate("z"), coordinate("y"), coordinate("x"), rows, :]
            send(block, SEMS[rnd, colour, phase, kind, None])
        elif "z" in whole:
            for plane in reversed(range(SIDE)) if planes is None else planes:
                panels(plane, SEMS[rnd, colour, phase, kind, plane])
        else:
            plane_here = self.shifted("z", source) if axis == "z" else self.me["z"]
            for plane in range(SIDE):
                pl.when(plane_here == plane)(
                    lambda plane=plane: panels(plane, SEMS[rnd, colour, phase, kind, None])
                )

    def start_own(self, rnd, colour, phase, planes=None):
        for kind in ("A+", "A-"):
            self.each(rnd, colour, phase, kind, 0, lambda copy: copy.start(), planes)

    def forward(self, rnd, colour, phase, planes=None):
        for kind, relay, source in (("A+", "F+", -1), ("A-", "F-", 1)):
            self.each(rnd, colour, phase, kind, source, lambda copy: copy.wait_recv(), planes)
            self.each(rnd, colour, phase, relay, source, lambda copy: copy.start(), planes)

    def finish(self, rnd, colour, phase, planes=None):
        for kind, source in (("F+", -2), ("F-", 2)):
            self.each(rnd, colour, phase, kind, source, lambda copy: copy.wait_recv(), planes)

    def event(self, name, rnd, colour, plane=None):
        planes = None if plane is None else (plane,)
        if name == "A1":
            self.start_own(rnd, colour, 0)
        elif name in ("F1", "F2", "F3"):
            self.forward(rnd, colour, int(name[1]) - 1, planes)
        elif name in ("A2", "A3"):
            phase = int(name[1]) - 1
            if planes is None or "z" in axes_of(rnd, colour)[: phase - 1]:
                self.finish(rnd, colour, phase - 1, planes)
            elif plane == SIDE - 1:
                self.finish(rnd, colour, phase - 1)
            self.start_own(rnd, colour, phase, planes)
        else:
            self.finish(rnd, colour, 2, planes)

    def drain(self):
        for rnd in range(ROUNDS):
            for colour in range(4):
                for phase in range(3):
                    for kind, source in (("A+", 0), ("A-", 0), ("F+", -1), ("F-", 1)):
                        self.each(rnd, colour, phase, kind, source, lambda copy: copy.wait_send())


LOW, MID, TOP = range(ROUNDS)
XYZ, YZX, ZXY = range(3)
Z0, Z1, Z2, Z3 = range(SIDE)
OPENING = (
    (
        ("A1", TOP, ZXY), ("A1", TOP, YZX), ("A1", TOP, XYZ), ("A1", LOW, XYZ), ("A1", MID, XYZ), ("A1", LOW, ZXY),
        ("A1", MID, YZX), ("F1", TOP, YZX), ("F1", TOP, ZXY), ("A1", LOW, YZX), ("A1", MID, ZXY), ("F1", MID, YZX),
        ("F1", LOW, XYZ), ("F1", LOW, ZXY), ("F1", TOP, XYZ), ("A2", TOP, ZXY, Z3), ("A2", TOP, YZX),
        ("A2", TOP, ZXY, Z2), ("A2", TOP, ZXY, Z0), ("F1", MID, XYZ), ("A2", TOP, ZXY, Z1),
    ),
    (
        ("F2", TOP, ZXY, Z3), ("A2", LOW, ZXY, Z3), ("A2", TOP, XYZ), ("A2", MID, YZX), ("F1", LOW, YZX),
        ("A2", LOW, ZXY, Z1), ("F2", TOP, YZX),
    ),
    (
        ("A2", MID, XYZ), ("F2", TOP, ZXY, Z1), ("F2", LOW, ZXY, Z3), ("F1", MID, ZXY), ("A2", LOW, ZXY, Z2),
        ("A2", LOW, YZX),
    ),
    (
        ("F2", TOP, XYZ), ("A3", TOP, ZXY, Z3),
    ),
    (
        ("A3", TOP, YZX, Z3), ("A3", LOW, ZXY, Z3), ("A2", LOW, ZXY, Z0), ("A3", TOP, YZX, Z2), ("A2", MID, ZXY, Z3),
        ("A2", MID, ZXY, Z0), ("A3", TOP, YZX, Z0), ("A2", MID, ZXY, Z2), ("F2", MID, YZX),
    ),
    (
        ("F2", LOW, ZXY, Z0), ("A1", MID, FACTOR), ("A3", TOP, ZXY, Z1), ("A2", MID, ZXY, Z1), ("F2", TOP, ZXY, Z2),
        ("F2", TOP, ZXY, Z0), ("A2", LOW, XYZ), ("A1", TOP, FACTOR), ("A3", TOP, XYZ), ("A3", MID, YZX, Z3),
        ("A1", LOW, FACTOR), ("F1", TOP, FACTOR), ("A3", TOP, ZXY, Z2), ("F1", MID, FACTOR), ("A3", TOP, YZX, Z1),
        ("F3", TOP, ZXY, Z1), ("F2", LOW, YZX), ("F3", TOP, ZXY, Z3), ("F3", TOP, YZX, Z0), ("A3", TOP, ZXY, Z0),
        ("F2", MID, ZXY, Z3), ("A2", TOP, FACTOR), ("F3", TOP, YZX, Z2), ("F2", MID, ZXY, Z2), ("A2", MID, FACTOR),
        ("F3", TOP, XYZ), ("F2", MID, ZXY, Z0), ("F1", LOW, FACTOR), ("F2", MID, XYZ), ("F3", MID, YZX, Z3),
        ("F2", TOP, FACTOR), ("F3", TOP, YZX, Z3), ("A3", MID, ZXY, Z3), ("D", TOP, YZX, Z2), ("F3", TOP, YZX, Z1),
        ("A3", MID, YZX, Z1), ("F2", MID, FACTOR), ("F3", TOP, ZXY, Z0), ("A3", MID, XYZ), ("D", TOP, XYZ),
        ("A2", LOW, FACTOR), ("A3", TOP, FACTOR), ("F3", MID, ZXY, Z3), ("F2", MID, ZXY, Z1), ("D", TOP, ZXY, Z1),
        ("A3", MID, YZX, Z2), ("D", TOP, YZX, Z0), ("D", MID, YZX, Z3), ("F2", LOW, FACTOR), ("A3", MID, FACTOR),
        ("A3", MID, YZX, Z0), ("D", TOP, YZX, Z1), ("F3", TOP, FACTOR), ("F3", TOP, ZXY, Z2), ("A3", MID, ZXY, Z1),
        ("F3", MID, FACTOR), ("F3", MID, YZX, Z2), ("D", TOP, ZXY, Z3), ("F2", LOW, XYZ), ("D", TOP, YZX, Z3),
        ("D", TOP, FACTOR), ("D", TOP, ZXY, Z0), ("A3", MID, ZXY, Z2), ("F3", MID, ZXY, Z1), ("F2", LOW, ZXY, Z2),
        ("A3", LOW, FACTOR), ("D", TOP, ZXY, Z2),
    ),
)
BEFORE_STEP = {
    1: (
        ("F3", MID, XYZ), ("D", MID, ZXY, Z3),
    ),
    3: (
        ("F3", MID, YZX, Z1), ("D", MID, FACTOR),
    ),
    4: (
        ("F3", MID, ZXY, Z2), ("D", MID, YZX, Z2), ("A3", LOW, YZX, Z3),
    ),
    5: (
        ("A3", MID, ZXY, Z0),
    ),
    6: (
        ("D", MID, ZXY, Z1),
    ),
    7: (
        ("F2", LOW, ZXY, Z1), ("D", MID, ZXY, Z2), ("A3", LOW, XYZ), ("F3", LOW, ZXY, Z3),
    ),
    8: (
        ("D", MID, YZX, Z1), ("F3", MID, YZX, Z0), ("D", MID, XYZ), ("A3", LOW, YZX, Z2), ("A3", LOW, ZXY, Z2),
        ("F3", MID, ZXY, Z0),
    ),
    11: (
        ("A3", LOW, YZX, Z1), ("F3", LOW, YZX, Z3),
    ),
    12: (
        ("A3", LOW, ZXY, Z1),
    ),
    13: (
        ("D", MID, ZXY, Z0), ("F3", LOW, FACTOR), ("D", MID, YZX, Z0), ("F3", LOW, XYZ),
    ),
    14: (
        ("F3", LOW, ZXY, Z2), ("D", LOW, ZXY, Z3), ("F3", LOW, YZX, Z2),
    ),
    15: (
        ("D", LOW, FACTOR),
    ),
    16: (
        ("A3", LOW, ZXY, Z0), ("D", LOW, XYZ), ("F3", LOW, ZXY, Z1), ("F3", LOW, YZX, Z1), ("D", LOW, YZX, Z3),
        ("A3", LOW, YZX, Z0),
    ),
    17: (
        ("D", LOW, YZX, Z2), ("D", LOW, ZXY, Z2),
    ),
    18: (
        ("D", LOW, YZX, Z1),
    ),
    19: (
        ("F3", LOW, ZXY, Z0),
    ),
    20: (
        ("D", LOW, ZXY, Z1), ("F3", LOW, YZX, Z0),
    ),
    22: (
        ("D", LOW, ZXY, Z0), ("D", LOW, YZX, Z0),
    ),
}


def nt(lhs, rhs):
    return lax.dot_general(lhs, rhs, (((1,), (1,)), ((), ())), precision=PRECISE, preferred_element_type=jnp.float32)


def nn(lhs, rhs):
    return lax.dot_general(lhs, rhs, (((1,), (0,)), ((), ())), precision=PRECISE, preferred_element_type=jnp.float32)


def merge_factor(t, gram):
    row = lax.broadcasted_iota(jnp.int32, (GROUP, GROUP), 0)
    column = lax.broadcasted_iota(jnp.int32, (GROUP, GROUP), 1)
    for width in (BLK, 2 * BLK, 4 * BLK):
        above = (row // (2 * width) == column // (2 * width)) & (row // width < column // width)
        t = t - nn(nn(t, jnp.where(above, gram, 0.0)), t)
    return t


def kernel(
    z_ref, v_ref, octet_ref, t_ref, out_ref, buf, factors, acc, peer, t_buf, rows_buf, gram, gram_peer, gram_pair,
    gram_parts, gram_full,
    send_sems, recv_sems, own_sems, z_keep_sems, z_send_sems, z_recv_sems, peer_send, peer_recv, octet_send, octet_recv, pair_send, pair_recv,
):
    gather = Gather(buf, factors, send_sems, recv_sems)
    me, core = gather.me, gather.core
    col = lax.axis_index("col")
    partner = (gather.kpt, col, 1 - core)
    seat = col % OCTET
    mates = {hop: (seat + hop) % OCTET for hop in range(1, OCTET)}

    def mate(hop):
        return (gather.kpt, col - seat + mates[hop], core)

    def to_mate(stage, hop, source, target):
        sem = stage * OCTET + hop
        return pltpu.make_async_remote_copy(
            src_ref=source, dst_ref=target, send_sem=octet_send.at[sem], recv_sem=octet_recv.at[sem],
            device_id=mate(hop), device_id_type=MESH,
        )

    def to_partner(sem, source, target):
        return pltpu.make_async_remote_copy(
            src_ref=source, dst_ref=target, send_sem=pair_send.at[sem], recv_sem=pair_recv.at[sem],
            device_id=partner, device_id_type=MESH,
        )

    own = []
    for rnd in range(ROUNDS):
        chunks = pl.ds(ROUND_BASE[rnd], CHUNKS - OCTET * rnd)
        rows = pl.ds(ROWS_BASE[rnd], ROUNDS - rnd)
        to_buf = (v_ref.at[rnd, pl.ds(OCTET * rnd, CHUNKS - OCTET * rnd)], buf.at[chunks, me["z"], me["y"], me["x"]])
        to_rows = (octet_ref.at[rnd, pl.ds(rnd, ROUNDS - rnd), seat], rows_buf.at[rows, seat])
        own.append(pltpu.make_async_copy(*to_buf, own_sems.at[rnd]))
        own.append(pltpu.make_async_copy(*to_rows, own_sems.at[ROUNDS + rnd]))
    for rnd in range(ROUNDS):
        own.append(pltpu.make_async_copy(t_ref.at[8 * rnd + col // OCTET], t_buf.at[rnd], own_sems.at[2 * ROUNDS + rnd]))
    for copy in own:
        copy.start()
    mine = pl.ds(core * (COLS // 2), COLS // 2)

    def z_chunk(half, chunk):
        return z_ref.at[:, pl.ds(pl.multiple_of((half * CHUNKS + chunk) * LANES, LANES), LANES)]

    def z_keep(chunk):
        return pltpu.make_async_copy(z_chunk(core, chunk), out_ref.at[chunk, mine], z_keep_sems.at[chunk])

    def z_give(chunk):
        return pltpu.make_async_remote_copy(
            src_ref=z_chunk(1 - core, chunk), dst_ref=out_ref.at[chunk, mine],
            send_sem=z_send_sems.at[chunk], recv_sem=z_recv_sems.at[chunk],
            device_id=partner, device_id_type=MESH,
        )

    def each_chunk(action):
        def body(chunk, _):
            action(chunk)
            return 0

        lax.fori_loop(0, CHUNKS, body, 0)

    each_chunk(lambda chunk: z_keep(chunk).start())

    barrier = pltpu.get_barrier_semaphore()
    peers = [gather.neighbour(axis, offset) for axis in "xyz" for offset in (1, -1)]
    peers += [mate(hop) for hop in mates] + [partner]
    for device in peers:
        pl.semaphore_signal(barrier, inc=1, device_id=device, device_id_type=MESH)
    pl.semaphore_wait(barrier, len(peers))

    halves = [to_partner(2 + rnd, factors.at[core, rnd], factors.at[core, rnd]) for rnd in range(ROUNDS)]

    def run(events):
        for event in events:
            gather.event(*event)
            if event[0] == "D" and event[2] == FACTOR:
                halves[event[1]].start()

    spread = [
        to_mate(
            rnd, hop, octet_ref.at[rnd, pl.ds(rnd, ROUNDS - rnd), at], rows_buf.at[pl.ds(ROWS_BASE[rnd], ROUNDS - rnd), seat]
        )
        for rnd in range(ROUNDS) for hop, at in mates.items()
    ]
    for copy in spread:
        copy.start()
    for copy in own:
        copy.wait()
    run(OPENING[0])
    each_chunk(lambda chunk: z_give(chunk).start())
    for copy in spread:
        copy.wait()
    for rnd, chunks in enumerate(((0, 1, 2), (3, 4), (5,))):
        panel = jnp.concatenate([rows_buf[chunk].reshape(GROUP, LANES) for chunk in chunks], axis=1)
        gram[:, :, rnd] = nt(panel, panel).reshape(OCTET, 2, SHARE, GROUP)
    pair = to_partner(0, gram.at[:, 1 - core], gram_peer)
    pair.start()
    run(OPENING[1])
    pair.wait()
    gram_pair[...] = gram[:, core] + gram_peer[...]
    scatter = [to_mate(ROUNDS, hop, gram_pair.at[at], gram_parts.at[seat]) for hop, at in mates.items()]
    for copy in scatter:
        copy.start()
    gram_parts[seat] = gram_pair[seat]
    run(OPENING[2])
    for copy in scatter:
        copy.wait()
    gram_full[core, seat] = jnp.sum(gram_parts[...], axis=0)
    collect = [to_mate(ROUNDS + 1, hop, gram_full.at[core, seat], gram_full.at[core, seat]) for hop in mates]
    for copy in collect:
        copy.start()
    run(OPENING[3])
    for copy in collect:
        copy.wait()
    pair = to_partner(1, gram_full.at[core], gram_full.at[core])
    pair.start()
    run(OPENING[4])
    pair.wait()

    def merge(rnd, _):
        row = lax.broadcasted_iota(jnp.int32, (GROUP, GROUP), 0)
        column = lax.broadcasted_iota(jnp.int32, (GROUP, GROUP), 1)
        diagonal = jnp.where(row // BLK == column // BLK, jnp.concatenate([t_buf[rnd]] * OCTET, axis=1), 0.0)
        pieces = [gram_full[half, at, rnd] for at in range(OCTET) for half in range(2)]
        t_mat = merge_factor(diagonal, jnp.concatenate(pieces, axis=0))
        for half in range(2):
            rows_buf[2 * rnd + half] = t_mat[:, half * LANES : (half + 1) * LANES].reshape(OCTET, BLK, LANES)
        factors[core, rnd, me["z"], me["y"], me["x"]] = rows_buf[2 * rnd + core, seat]
        return 0

    lax.fori_loop(0, ROUNDS, merge, 0)
    run(OPENING[5])
    each_chunk(lambda chunk: z_keep(chunk).wait())
    each_chunk(lambda chunk: z_give(chunk).wait())

    def over_tiles(first, body):
        count = CHUNKS // 2 - first
        pl.when(count % 2 == 1)(lambda: body(first, 1))
        pl.when(count % 4 >= 2)(lambda: body(first + count % 2, 2))

        def four(i, _):
            body(first + count % 4 + 4 * i, 4)
            return 0

        lax.fori_loop(0, count // 4, four, 0)

    def step(idx, _):
        for at, events in BEFORE_STEP.items():
            @pl.when(idx == at)
            def _(events=events):
                run(events)

        for needed in range(ROUNDS):
            pl.when(idx == 16 - 8 * needed)(lambda needed=needed: halves[needed].wait())

        group = STEPS - 1 - idx
        rnd = group // 8
        plane = (group % 8) // 2
        pair_row = (group % 2) * 2
        slot = idx % 2
        shift = 16 * rnd - 4 * rnd * (rnd - 1)
        first = 4 * rnd + plane

        def tile(w):
            halves = [
                buf[shift + 2 * w + half, plane, pl.ds(pair_row, 2), :, :, :].reshape(GROUP, LANES) for half in range(2)
            ]
            return jnp.concatenate(halves, axis=1)

        def z_tile(w):
            return jnp.concatenate([out_ref[2 * w], out_ref[2 * w + 1]], axis=1)

        acc[...] = jnp.zeros_like(acc)

        def project(w, count):
            z = jnp.concatenate([z_tile(w + i) for i in range(count)], axis=1)
            acc[...] += nt(z, jnp.concatenate([tile(w + i) for i in range(count)], axis=1))

        over_tiles(first, project)

        exchange = pltpu.make_async_remote_copy(
            src_ref=acc, dst_ref=peer.at[slot], send_sem=peer_send.at[slot], recv_sem=peer_recv.at[slot],
            device_id=partner, device_id_type=MESH,
        )
        exchange.start()

        t_mat = jnp.concatenate(
            [factors[half, rnd, plane, pl.ds(pair_row, 2)].reshape(GROUP, LANES) for half in range(2)], axis=1
        )
        exchange.wait()
        w_full = nt(acc[...] + peer[slot], t_mat)

        def update(w, count):
            delta = nn(w_full, jnp.concatenate([tile(w + i) for i in range(count)], axis=1))
            for i in range(2 * count):
                out_ref[2 * w + i] -= delta[:, i * LANES : (i + 1) * LANES]

        over_tiles(first, update)
        return 0

    lax.fori_loop(0, STEPS, step, 0)
    gather.drain()


def apply_panels(z, v, t):
    def vmem(*shape):
        return pltpu.VMEM(shape, jnp.float32)

    return pl.pallas_call(
        kernel,
        out_shape=jax.ShapeDtypeStruct((CHUNKS, COLS, LANES), jnp.float32),
        in_specs=[pl.BlockSpec(memory_space=pl.ANY)] * 4,
        out_specs=pl.BlockSpec(memory_space=pltpu.VMEM),
        scratch_shapes=[
            vmem(SLOTS, SIDE, SIDE, SIDE, BLK, LANES),
            vmem(2, ROUNDS, SIDE, SIDE, SIDE, BLK, LANES),
            vmem(COLS, GROUP),
            vmem(2, COLS, GROUP),
            vmem(ROUNDS, GROUP, BLK),
            vmem(SLOTS // OCTET, OCTET, BLK, LANES),
            vmem(OCTET, 2, ROUNDS, SHARE, GROUP),
            vmem(OCTET, ROUNDS, SHARE, GROUP),
            vmem(OCTET, ROUNDS, SHARE, GROUP),
            vmem(OCTET, ROUNDS, SHARE, GROUP),
            vmem(2, OCTET, ROUNDS, SHARE, GROUP),
            pltpu.SemaphoreType.DMA((len(SEMS),)),
            pltpu.SemaphoreType.DMA((len(SEMS),)),
            pltpu.SemaphoreType.DMA((3 * ROUNDS,)),
            pltpu.SemaphoreType.DMA((CHUNKS,)),
            pltpu.SemaphoreType.DMA((CHUNKS,)),
            pltpu.SemaphoreType.DMA((CHUNKS,)),
            pltpu.SemaphoreType.DMA((2,)),
            pltpu.SemaphoreType.DMA((2,)),
            pltpu.SemaphoreType.DMA(((ROUNDS + 2) * OCTET,)),
            pltpu.SemaphoreType.DMA(((ROUNDS + 2) * OCTET,)),
            pltpu.SemaphoreType.DMA((2 + ROUNDS,)),
            pltpu.SemaphoreType.DMA((2 + ROUNDS,)),
        ],
        compiler_params=pltpu.CompilerParams(collective_id=0, has_side_effects=True, vmem_limit_bytes=67043328),
        name="apply_panels",
    )(z, v, v.reshape(ROUNDS, CHUNKS // OCTET, OCTET, BLK, LANES), t)


def solution(mesh):
    def local_run(z_cols, v_local, t_local):
        z = z_cols.T
        v = v_local.reshape(CHUNKS, LANES, ROUNDS, BLK).transpose(2, 0, 3, 1)
        out = apply_panels(z, v, t_local.reshape(STEPS, GROUP, BLK))
        return out.transpose(0, 2, 1).reshape(CHUNKS * LANES, COLS)

    return jax.shard_map(
        local_run,
        mesh=mesh,
        in_specs=(P("kpt", ("col", "row")), P(("kpt", "row"), "col"), P("kpt", None, None)),
        out_specs=P(("kpt", "row"), "col"),
        check_vma=False,
    )
```

```python
import jax
import jax.numpy as jnp
from jax import lax
from jax.experimental import pallas as pl
from jax.experimental.pallas import tpu as pltpu
from jax.sharding import PartitionSpec as P

PRECISE = lax.Precision.HIGHEST
MESH = pl.DeviceIdType.MESH

SIDE = 4
BLK = 32
ROUNDS = 3
LANES = 128
CHUNKS = 24
GROUP = 256
STEPS = 24
COLS = 64

ORDER = (("x", "y", "z"), ("y", "z", "x"), ("z", "x", "y"))
SHARES = {
    24: (4, 10, 10), 22: (4, 9, 9), 20: (4, 8, 8), 18: (4, 7, 7),
    16: (4, 6, 6), 14: (4, 5, 5), 12: (4, 4, 4), 10: (4, 3, 3),
    8: (2, 3, 3), 6: (2, 2, 2), 4: (2, 1, 1), 2: (1, 1, 0),
}
ROWS_BASE = (0, 3, 5)
ROUND_BASE = (0, 24, 40)
SLOTS = 48
KINDS = ("A+", "A-", "F+", "F-")
FACTOR = 3
OCTET = 8
SHARE = 16


def axes_of(rnd, colour):
    return ORDER[rnd if colour == FACTOR else colour]


def part(rnd, z_src, colour):
    first = 8 * rnd + 2 * z_src
    shares = SHARES[CHUNKS - first]
    return ROUND_BASE[rnd] + first - 8 * rnd + sum(shares[:colour]), shares[colour]


def sem_table():
    table = {}
    for rnd in range(ROUNDS):
        for colour in range(4):
            for phase in range(3):
                planes = range(SIDE) if colour != FACTOR and "z" in ORDER[colour][:phase] else (None,)
                for kind in KINDS:
                    for plane in planes:
                        table[rnd, colour, phase, kind, plane] = len(table)
    return table


SEMS = sem_table()


class Gather:
    def __init__(self, buf, factors, send_sems, recv_sems):
        col = lax.axis_index("col")
        self.kpt, self.core = lax.axis_index("kpt"), lax.axis_index("row")
        self.me = {"z": col // 16, "y": (col // 4) % 4, "x": col % 4}
        self.buf, self.factors, self.send_sems, self.recv_sems = buf, factors, send_sems, recv_sems
        self.at = {(axis, offset): (self.me[axis] + offset) % SIDE for axis in "xyz" for offset in (1, 2, 3)}
        self.peer = {(axis, offset): self.find(axis, offset) for axis in "xyz" for offset in (1, 3)}

    def find(self, axis, offset):
        at = dict(self.me)
        at[axis] = self.at[axis, offset]
        return (self.kpt, at["z"] * 16 + at["y"] * 4 + at["x"], self.core)

    def shifted(self, axis, offset):
        return self.me[axis] if offset == 0 else self.at[axis, offset % SIDE]

    def neighbour(self, axis, offset):
        return self.peer[axis, offset % SIDE]

    def each(self, rnd, colour, phase, kind, source, fn, planes=None):
        axis = axes_of(rnd, colour)[phase]
        whole = axes_of(rnd, colour)[:phase]
        rows = {"A+": pl.ds(0, BLK), "A-": pl.ds(0, BLK), "F+": pl.ds(0, BLK // 2), "F-": pl.ds(BLK // 2, BLK // 2)}[kind]
        target = self.neighbour(axis, 1 if kind[1] == "+" else -1)

        def coordinate(name):
            if name in whole:
                return slice(None)
            return self.shifted(name, source) if name == axis else self.me[name]

        def send(block, sem):
            fn(
                pltpu.make_async_remote_copy(
                    src_ref=block, dst_ref=block,
                    send_sem=self.send_sems.at[sem], recv_sem=self.recv_sems.at[sem],
                    device_id=target, device_id_type=MESH,
                )
            )

        def panels(plane, sem):
            slot, count = part(rnd, plane, colour)
            if count:
                send(self.buf.at[pl.ds(slot, count), plane, coordinate("y"), coordinate("x"), rows, :], sem)

        if colour == FACTOR:
            block = self.factors.at[self.core, rnd, coordinate("z"), coordinate("y"), coordinate("x"), rows, :]
            send(block, SEMS[rnd, colour, phase, kind, None])
        elif "z" in whole:
            for plane in reversed(range(SIDE)) if planes is None else planes:
                panels(plane, SEMS[rnd, colour, phase, kind, plane])
        else:
            plane_here = self.shifted("z", source) if axis == "z" else self.me["z"]
            for plane in range(SIDE):
                pl.when(plane_here == plane)(
                    lambda plane=plane: panels(plane, SEMS[rnd, colour, phase, kind, None])
                )

    def start_own(self, rnd, colour, phase, planes=None):
        for kind in ("A+", "A-"):
            self.each(rnd, colour, phase, kind, 0, lambda copy: copy.start(), planes)

    def forward(self, rnd, colour, phase, planes=None):
        for kind, relay, source in (("A+", "F+", -1), ("A-", "F-", 1)):
            self.each(rnd, colour, phase, kind, source, lambda copy: copy.wait_recv(), planes)
            self.each(rnd, colour, phase, relay, source, lambda copy: copy.start(), planes)

    def finish(self, rnd, colour, phase, planes=None):
        for kind, source in (("F+", -2), ("F-", 2)):
            self.each(rnd, colour, phase, kind, source, lambda copy: copy.wait_recv(), planes)

    def event(self, name, rnd, colour, plane=None):
        planes = None if plane is None else (plane,)
        if name == "A1":
            self.start_own(rnd, colour, 0)
        elif name in ("F1", "F2", "F3"):
            self.forward(rnd, colour, int(name[1]) - 1, planes)
        elif name in ("A2", "A3"):
            phase = int(name[1]) - 1
            if planes is None or "z" in axes_of(rnd, colour)[: phase - 1]:
                self.finish(rnd, colour, phase - 1, planes)
            elif plane == SIDE - 1:
                self.finish(rnd, colour, phase - 1)
            self.start_own(rnd, colour, phase, planes)
        else:
            self.finish(rnd, colour, 2, planes)

    def drain(self):
        for rnd in range(ROUNDS):
            for colour in range(4):
                for phase in range(3):
                    for kind, source in (("A+", 0), ("A-", 0), ("F+", -1), ("F-", 1)):
                        self.each(rnd, colour, phase, kind, source, lambda copy: copy.wait_send())


LOW, MID, TOP = range(ROUNDS)
XYZ, YZX, ZXY = range(3)
Z0, Z1, Z2, Z3 = range(SIDE)
OPENING = (
    (
        ("A1", TOP, ZXY), ("A1", TOP, YZX), ("A1", TOP, XYZ), ("A1", MID, ZXY), ("A1", LOW, XYZ), ("A1", LOW, ZXY),
        ("A1", MID, YZX), ("A1", MID, XYZ), ("F1", TOP, YZX), ("F1", TOP, ZXY), ("A1", LOW, YZX),
    ),
    (
        ("F1", MID, ZXY), ("F1", MID, XYZ), ("A2", TOP, YZX), ("A2", TOP, ZXY, Z3), ("A2", MID, ZXY, Z3),
        ("A2", TOP, ZXY, Z0), ("F1", LOW, ZXY), ("F1", MID, YZX), ("A2", TOP, ZXY, Z2), ("A2", MID, ZXY, Z1),
    ),
    (
        ("F1", LOW, YZX), ("A2", TOP, ZXY, Z1), ("F2", MID, ZXY, Z3), ("A2", MID, XYZ), ("F2", TOP, YZX),
        ("A2", MID, YZX),
    ),
    (
        ("F2", TOP, ZXY, Z0), ("F2", TOP, ZXY, Z3), ("F1", TOP, XYZ), ("F2", TOP, ZXY, Z2), ("A2", LOW, ZXY, Z3),
        ("A3", MID, ZXY, Z3),
    ),
    (
        ("A3", TOP, ZXY, Z3), ("A2", MID, ZXY, Z2), ("A3", TOP, YZX, Z3), ("A2", TOP, XYZ), ("A2", LOW, ZXY, Z2),
        ("A3", TOP, ZXY, Z0), ("A3", TOP, YZX, Z0), ("A2", LOW, YZX), ("A2", LOW, ZXY, Z1),
    ),
    (
        ("A1", TOP, FACTOR), ("F2", LOW, ZXY, Z3), ("A3", TOP, ZXY, Z2), ("F2", MID, YZX), ("A1", MID, FACTOR),
        ("F2", MID, ZXY, Z2), ("F2", MID, XYZ), ("F3", TOP, ZXY, Z3), ("F1", LOW, XYZ), ("A2", MID, ZXY, Z0),
        ("F2", MID, ZXY, Z1), ("A3", TOP, YZX, Z1), ("F1", MID, FACTOR), ("F2", TOP, XYZ), ("F3", TOP, YZX, Z0),
        ("F3", MID, ZXY, Z3), ("A2", MID, FACTOR), ("F3", TOP, YZX, Z3), ("A1", LOW, FACTOR), ("F3", TOP, ZXY, Z0),
        ("A3", TOP, YZX, Z2), ("F1", TOP, FACTOR), ("F2", TOP, ZXY, Z1), ("A3", MID, ZXY, Z2), ("A3", TOP, XYZ),
        ("A3", MID, YZX, Z3), ("F2", MID, FACTOR), ("F3", TOP, ZXY, Z2), ("F1", LOW, FACTOR), ("A3", LOW, ZXY, Z3),
        ("A2", TOP, FACTOR), ("A3", MID, YZX, Z2), ("F3", TOP, XYZ), ("A3", MID, XYZ), ("F2", TOP, FACTOR),
        ("D", TOP, ZXY, Z2), ("A3", MID, YZX, Z1), ("D", TOP, YZX, Z3), ("F3", TOP, YZX, Z2), ("F3", TOP, YZX, Z1),
        ("D", MID, ZXY, Z3), ("A3", TOP, ZXY, Z1), ("A3", TOP, FACTOR), ("D", TOP, XYZ), ("F2", LOW, YZX),
        ("A3", MID, FACTOR), ("F3", TOP, ZXY, Z1), ("F3", MID, YZX, Z1), ("D", TOP, ZXY, Z3), ("F3", TOP, FACTOR),
        ("A2", LOW, FACTOR), ("D", TOP, YZX, Z2), ("F3", MID, YZX, Z3), ("D", TOP, FACTOR), ("A2", LOW, XYZ),
        ("D", TOP, ZXY, Z1), ("F2", LOW, ZXY, Z1), ("D", TOP, YZX, Z0), ("F3", MID, YZX, Z2), ("A3", MID, ZXY, Z1),
        ("D", TOP, YZX, Z1), ("A3", MID, YZX, Z0), ("D", TOP, ZXY, Z0),
    ),
)
BEFORE_STEP = {
    3: (
        ("F3", MID, FACTOR), ("F2", MID, ZXY, Z0),
    ),
    4: (
        ("F2", LOW, FACTOR), ("F3", LOW, ZXY, Z3),
    ),
    5: (
        ("F3", MID, ZXY, Z1), ("F3", MID, ZXY, Z2), ("F2", LOW, ZXY, Z2), ("D", MID, YZX, Z2), ("F3", MID, XYZ),
        ("F2", LOW, XYZ),
    ),
    6: (
        ("D", MID, FACTOR), ("D", MID, YZX, Z3), ("F3", MID, YZX, Z0), ("A3", LOW, YZX, Z3), ("A3", LOW, FACTOR),
        ("D", MID, YZX, Z1),
    ),
    7: (
        ("A3", MID, ZXY, Z0), ("D", MID, ZXY, Z1),
    ),
    8: (
        ("D", MID, YZX, Z0), ("D", MID, ZXY, Z2), ("A3", LOW, YZX, Z2), ("A2", LOW, ZXY, Z0), ("D", LOW, ZXY, Z3),
        ("A3", LOW, ZXY, Z2), ("A3", LOW, XYZ), ("D", MID, XYZ),
    ),
    11: (
        ("F3", MID, ZXY, Z0), ("A3", LOW, ZXY, Z1), ("A3", LOW, YZX, Z1),
    ),
    12: (
        ("F3", LOW, FACTOR),
    ),
    14: (
        ("F3", LOW, XYZ), ("F3", LOW, ZXY, Z2), ("F3", LOW, YZX, Z3), ("D", MID, ZXY, Z0), ("F2", LOW, ZXY, Z0),
    ),
    15: (
        ("F3", LOW, YZX, Z2), ("F3", LOW, ZXY, Z1), ("D", LOW, FACTOR),
    ),
    16: (
        ("A3", LOW, ZXY, Z0), ("A3", LOW, YZX, Z0), ("D", LOW, YZX, Z3), ("D", LOW, ZXY, Z2), ("F3", LOW, YZX, Z1),
        ("D", LOW, XYZ),
    ),
    18: (
        ("D", LOW, YZX, Z2),
    ),
    19: (
        ("F3", LOW, ZXY, Z0),
    ),
    20: (
        ("D", LOW, YZX, Z1), ("F3", LOW, YZX, Z0), ("D", LOW, ZXY, Z1),
    ),
    22: (
        ("D", LOW, ZXY, Z0), ("D", LOW, YZX, Z0),
    ),
}


def nt(lhs, rhs):
    return lax.dot_general(lhs, rhs, (((1,), (1,)), ((), ())), precision=PRECISE, preferred_element_type=jnp.float32)


def nn(lhs, rhs):
    return lax.dot_general(lhs, rhs, (((1,), (0,)), ((), ())), precision=PRECISE, preferred_element_type=jnp.float32)


def merge_factor(t, gram):
    row = lax.broadcasted_iota(jnp.int32, (GROUP, GROUP), 0)
    column = lax.broadcasted_iota(jnp.int32, (GROUP, GROUP), 1)
    for width in (BLK, 2 * BLK, 4 * BLK):
        above = (row // (2 * width) == column // (2 * width)) & (row // width < column // width)
        t = t - nn(nn(t, jnp.where(above, gram, 0.0)), t)
    return t


def kernel(
    z_ref, v_ref, octet_ref, t_ref, out_ref, buf, factors, acc, peer, t_buf, rows_buf, gram, gram_peer, gram_pair,
    gram_parts, gram_full,
    send_sems, recv_sems, own_sems, z_keep_sems, z_send_sems, z_recv_sems, peer_send, peer_recv, octet_send, octet_recv, pair_send, pair_recv,
):
    gather = Gather(buf, factors, send_sems, recv_sems)
    me, core = gather.me, gather.core
    col = lax.axis_index("col")
    partner = (gather.kpt, col, 1 - core)
    seat = col % OCTET
    mates = {hop: (seat + hop) % OCTET for hop in range(1, OCTET)}

    def mate(hop):
        return (gather.kpt, col - seat + mates[hop], core)

    def to_mate(stage, hop, source, target):
        sem = stage * OCTET + hop
        return pltpu.make_async_remote_copy(
            src_ref=source, dst_ref=target, send_sem=octet_send.at[sem], recv_sem=octet_recv.at[sem],
            device_id=mate(hop), device_id_type=MESH,
        )

    def to_partner(sem, source, target):
        return pltpu.make_async_remote_copy(
            src_ref=source, dst_ref=target, send_sem=pair_send.at[sem], recv_sem=pair_recv.at[sem],
            device_id=partner, device_id_type=MESH,
        )

    own = []
    for rnd in range(ROUNDS):
        chunks = pl.ds(ROUND_BASE[rnd], CHUNKS - OCTET * rnd)
        rows = pl.ds(ROWS_BASE[rnd], ROUNDS - rnd)
        to_buf = (v_ref.at[rnd, pl.ds(OCTET * rnd, CHUNKS - OCTET * rnd)], buf.at[chunks, me["z"], me["y"], me["x"]])
        to_rows = (octet_ref.at[rnd, pl.ds(rnd, ROUNDS - rnd), seat], rows_buf.at[rows, seat])
        own.append(pltpu.make_async_copy(*to_buf, own_sems.at[rnd]))
        own.append(pltpu.make_async_copy(*to_rows, own_sems.at[ROUNDS + rnd]))
    for rnd in range(ROUNDS):
        own.append(pltpu.make_async_copy(t_ref.at[8 * rnd + col // OCTET], t_buf.at[rnd], own_sems.at[2 * ROUNDS + rnd]))
    for copy in own:
        copy.start()
    mine = pl.ds(core * (COLS // 2), COLS // 2)

    def z_chunk(half, chunk):
        return z_ref.at[:, pl.ds(pl.multiple_of((half * CHUNKS + chunk) * LANES, LANES), LANES)]

    def z_keep(chunk):
        return pltpu.make_async_copy(z_chunk(core, chunk), out_ref.at[chunk, mine], z_keep_sems.at[chunk])

    def z_give(chunk):
        return pltpu.make_async_remote_copy(
            src_ref=z_chunk(1 - core, chunk), dst_ref=out_ref.at[chunk, mine],
            send_sem=z_send_sems.at[chunk], recv_sem=z_recv_sems.at[chunk],
            device_id=partner, device_id_type=MESH,
        )

    def each_chunk(action):
        def body(chunk, _):
            action(chunk)
            return 0

        lax.fori_loop(0, CHUNKS, body, 0)

    each_chunk(lambda chunk: z_keep(chunk).start())

    barrier = pltpu.get_barrier_semaphore()
    peers = [gather.neighbour(axis, offset) for axis in "xyz" for offset in (1, -1)]
    peers += [mate(hop) for hop in mates] + [partner]
    for device in peers:
        pl.semaphore_signal(barrier, inc=1, device_id=device, device_id_type=MESH)
    pl.semaphore_wait(barrier, len(peers))

    halves = [to_partner(2 + rnd, factors.at[core, rnd], factors.at[core, rnd]) for rnd in range(ROUNDS)]

    def run(events):
        for event in events:
            gather.event(*event)
            if event[0] == "D" and event[2] == FACTOR:
                halves[event[1]].start()

    spread = [
        to_mate(
            rnd, hop, octet_ref.at[rnd, pl.ds(rnd, ROUNDS - rnd), at], rows_buf.at[pl.ds(ROWS_BASE[rnd], ROUNDS - rnd), seat]
        )
        for rnd in range(ROUNDS) for hop, at in mates.items()
    ]
    for copy in spread:
        copy.start()
    for copy in own:
        copy.wait()
    run(OPENING[0])
    each_chunk(lambda chunk: z_give(chunk).start())
    for copy in spread:
        copy.wait()
    for rnd, chunks in enumerate(((0, 1, 2), (3, 4), (5,))):
        panel = jnp.concatenate([rows_buf[chunk].reshape(GROUP, LANES) for chunk in chunks], axis=1)
        gram[:, :, rnd] = nt(panel, panel).reshape(OCTET, 2, SHARE, GROUP)
    pair = to_partner(0, gram.at[:, 1 - core], gram_peer)
    pair.start()
    run(OPENING[1])
    pair.wait()
    gram_pair[...] = gram[:, core] + gram_peer[...]
    scatter = [to_mate(ROUNDS, hop, gram_pair.at[at], gram_parts.at[seat]) for hop, at in mates.items()]
    for copy in scatter:
        copy.start()
    gram_parts[seat] = gram_pair[seat]
    run(OPENING[2])
    for copy in scatter:
        copy.wait()
    gram_full[core, seat] = jnp.sum(gram_parts[...], axis=0)
    collect = [to_mate(ROUNDS + 1, hop, gram_full.at[core, seat], gram_full.at[core, seat]) for hop in mates]
    for copy in collect:
        copy.start()
    run(OPENING[3])
    for copy in collect:
        copy.wait()
    pair = to_partner(1, gram_full.at[core], gram_full.at[core])
    pair.start()
    run(OPENING[4])
    pair.wait()

    def merge(rnd, _):
        row = lax.broadcasted_iota(jnp.int32, (GROUP, GROUP), 0)
        column = lax.broadcasted_iota(jnp.int32, (GROUP, GROUP), 1)
        diagonal = jnp.where(row // BLK == column // BLK, jnp.concatenate([t_buf[rnd]] * OCTET, axis=1), 0.0)
        pieces = [gram_full[half, at, rnd] for at in range(OCTET) for half in range(2)]
        t_mat = merge_factor(diagonal, jnp.concatenate(pieces, axis=0)).T
        for half in range(2):
            rows_buf[2 * rnd + half] = t_mat[:, half * LANES : (half + 1) * LANES].reshape(OCTET, BLK, LANES)
        factors[core, rnd, me["z"], me["y"], me["x"]] = rows_buf[2 * rnd + core, seat]
        return 0

    lax.fori_loop(0, ROUNDS, merge, 0)
    run(OPENING[5])
    each_chunk(lambda chunk: z_keep(chunk).wait())
    each_chunk(lambda chunk: z_give(chunk).wait())

    def over_tiles(first, body):
        count = CHUNKS // 2 - first
        pl.when(count % 2 == 1)(lambda: body(first, 1))
        pl.when(count % 4 >= 2)(lambda: body(first + count % 2, 2))

        def four(i, _):
            body(first + count % 4 + 4 * i, 4)
            return 0

        lax.fori_loop(0, count // 4, four, 0)

    def step(idx, _):
        for at, events in BEFORE_STEP.items():
            @pl.when(idx == at)
            def _(events=events):
                run(events)

        for needed in range(ROUNDS):
            pl.when(idx == 16 - 8 * needed)(lambda needed=needed: halves[needed].wait())

        group = STEPS - 1 - idx
        rnd = group // 8
        plane = (group % 8) // 2
        pair_row = (group % 2) * 2
        slot = idx % 2
        shift = 16 * rnd - 4 * rnd * (rnd - 1)
        first = 4 * rnd + plane

        def tile(w):
            halves = [
                buf[shift + 2 * w + half, plane, pl.ds(pair_row, 2), :, :, :].reshape(GROUP, LANES) for half in range(2)
            ]
            return jnp.concatenate(halves, axis=1)

        def z_tile(w):
            return jnp.concatenate([out_ref[2 * w], out_ref[2 * w + 1]], axis=1)

        acc[...] = jnp.zeros_like(acc)

        def project(w, count):
            z = jnp.concatenate([z_tile(w + i) for i in range(count)], axis=1)
            acc[...] += nt(z, jnp.concatenate([tile(w + i) for i in range(count)], axis=1))

        over_tiles(first, project)

        exchange = pltpu.make_async_remote_copy(
            src_ref=acc, dst_ref=peer.at[slot], send_sem=peer_send.at[slot], recv_sem=peer_recv.at[slot],
            device_id=partner, device_id_type=MESH,
        )
        exchange.start()

        t_mat = jnp.concatenate(
            [factors[half, rnd, plane, pl.ds(pair_row, 2)].reshape(GROUP, LANES) for half in range(2)], axis=1
        )
        exchange.wait()
        w_full = nn(acc[...] + peer[slot], t_mat)

        def update(w, count):
            delta = nn(w_full, jnp.concatenate([tile(w + i) for i in range(count)], axis=1))
            for i in range(2 * count):
                out_ref[2 * w + i] -= delta[:, i * LANES : (i + 1) * LANES]

        over_tiles(first, update)
        return 0

    lax.fori_loop(0, STEPS, step, 0)
    gather.drain()


def apply_panels(z, v, t):
    def vmem(*shape):
        return pltpu.VMEM(shape, jnp.float32)

    return pl.pallas_call(
        kernel,
        out_shape=jax.ShapeDtypeStruct((CHUNKS, COLS, LANES), jnp.float32),
        in_specs=[pl.BlockSpec(memory_space=pl.ANY)] * 4,
        out_specs=pl.BlockSpec(memory_space=pltpu.VMEM),
        scratch_shapes=[
            vmem(SLOTS, SIDE, SIDE, SIDE, BLK, LANES),
            vmem(2, ROUNDS, SIDE, SIDE, SIDE, BLK, LANES),
            vmem(COLS, GROUP),
            vmem(2, COLS, GROUP),
            vmem(ROUNDS, GROUP, BLK),
            vmem(SLOTS // OCTET, OCTET, BLK, LANES),
            vmem(OCTET, 2, ROUNDS, SHARE, GROUP),
            vmem(OCTET, ROUNDS, SHARE, GROUP),
            vmem(OCTET, ROUNDS, SHARE, GROUP),
            vmem(OCTET, ROUNDS, SHARE, GROUP),
            vmem(2, OCTET, ROUNDS, SHARE, GROUP),
            pltpu.SemaphoreType.DMA((len(SEMS),)),
            pltpu.SemaphoreType.DMA((len(SEMS),)),
            pltpu.SemaphoreType.DMA((3 * ROUNDS,)),
            pltpu.SemaphoreType.DMA((CHUNKS,)),
            pltpu.SemaphoreType.DMA((CHUNKS,)),
            pltpu.SemaphoreType.DMA((CHUNKS,)),
            pltpu.SemaphoreType.DMA((2,)),
            pltpu.SemaphoreType.DMA((2,)),
            pltpu.SemaphoreType.DMA(((ROUNDS + 2) * OCTET,)),
            pltpu.SemaphoreType.DMA(((ROUNDS + 2) * OCTET,)),
            pltpu.SemaphoreType.DMA((2 + ROUNDS,)),
            pltpu.SemaphoreType.DMA((2 + ROUNDS,)),
        ],
        compiler_params=pltpu.CompilerParams(collective_id=0, has_side_effects=True, vmem_limit_bytes=67043328),
        name="apply_panels",
    )(z, v, v.reshape(ROUNDS, CHUNKS // OCTET, OCTET, BLK, LANES), t)


def solution(mesh):
    def local_run(z_cols, v_local, t_local):
        z = z_cols.T
        v = v_local.reshape(CHUNKS, LANES, ROUNDS, BLK).transpose(2, 0, 3, 1)
        out = apply_panels(z, v, t_local.reshape(STEPS, GROUP, BLK))
        return out.transpose(0, 2, 1).reshape(CHUNKS * LANES, COLS)

    return jax.shard_map(
        local_run,
        mesh=mesh,
        in_specs=(P("kpt", ("col", "row")), P(("kpt", "row"), "col"), P("kpt", None, None)),
        out_specs=P(("kpt", "row"), "col"),
        check_vma=False,
    )
```

```python
import jax
import jax.numpy as jnp
from jax import lax
from jax.experimental import pallas as pl
from jax.experimental.pallas import tpu as pltpu
from jax.sharding import PartitionSpec as P

PRECISE = lax.Precision.HIGHEST
MESH = pl.DeviceIdType.MESH

SIDE = 4
BLK = 32
ROUNDS = 3
LANES = 128
CHUNKS = 24
GROUP = 256
STEPS = 24
COLS = 64

ORDER = (("x", "y", "z"), ("y", "z", "x"), ("z", "x", "y"))
SHARES = {
    24: (4, 10, 10), 22: (4, 9, 9), 20: (4, 8, 8), 18: (4, 7, 7),
    16: (4, 6, 6), 14: (4, 5, 5), 12: (4, 4, 4), 10: (4, 3, 3),
    8: (2, 3, 3), 6: (2, 2, 2), 4: (2, 1, 1), 2: (1, 1, 0),
}
ROWS_BASE = (0, 3, 5)
ROUND_BASE = (0, 24, 40)
SLOTS = 48
KINDS = ("A+", "A-", "F+", "F-")
FACTOR = 3
OCTET = 8
SHARE = 16


def axes_of(rnd, colour):
    return ORDER[rnd if colour == FACTOR else colour]


def part(rnd, z_src, colour):
    first = 8 * rnd + 2 * z_src
    shares = SHARES[CHUNKS - first]
    return ROUND_BASE[rnd] + first - 8 * rnd + sum(shares[:colour]), shares[colour]


def sem_table():
    table = {}
    for rnd in range(ROUNDS):
        for colour in range(4):
            for phase in range(3):
                planes = range(SIDE) if colour != FACTOR and "z" in ORDER[colour][:phase] else (None,)
                for kind in KINDS:
                    for plane in planes:
                        table[rnd, colour, phase, kind, plane] = len(table)
    return table


SEMS = sem_table()


class Gather:
    def __init__(self, buf, factors, send_sems, recv_sems):
        col = lax.axis_index("col")
        self.kpt, self.core = lax.axis_index("kpt"), lax.axis_index("row")
        self.me = {"z": col // 16, "y": (col // 4) % 4, "x": col % 4}
        self.buf, self.factors, self.send_sems, self.recv_sems = buf, factors, send_sems, recv_sems
        self.at = {(axis, offset): (self.me[axis] + offset) % SIDE for axis in "xyz" for offset in (1, 2, 3)}
        self.peer = {(axis, offset): self.find(axis, offset) for axis in "xyz" for offset in (1, 3)}

    def find(self, axis, offset):
        at = dict(self.me)
        at[axis] = self.at[axis, offset]
        return (self.kpt, at["z"] * 16 + at["y"] * 4 + at["x"], self.core)

    def shifted(self, axis, offset):
        return self.me[axis] if offset == 0 else self.at[axis, offset % SIDE]

    def neighbour(self, axis, offset):
        return self.peer[axis, offset % SIDE]

    def each(self, rnd, colour, phase, kind, source, fn, planes=None):
        axis = axes_of(rnd, colour)[phase]
        whole = axes_of(rnd, colour)[:phase]
        rows = {"A+": pl.ds(0, BLK), "A-": pl.ds(0, BLK), "F+": pl.ds(0, BLK // 2), "F-": pl.ds(BLK // 2, BLK // 2)}[kind]
        target = self.neighbour(axis, 1 if kind[1] == "+" else -1)

        def coordinate(name):
            if name in whole:
                return slice(None)
            return self.shifted(name, source) if name == axis else self.me[name]

        def send(block, sem):
            fn(
                pltpu.make_async_remote_copy(
                    src_ref=block, dst_ref=block,
                    send_sem=self.send_sems.at[sem], recv_sem=self.recv_sems.at[sem],
                    device_id=target, device_id_type=MESH,
                )
            )

        def panels(plane, sem):
            slot, count = part(rnd, plane, colour)
            if count:
                send(self.buf.at[pl.ds(slot, count), plane, coordinate("y"), coordinate("x"), rows, :], sem)

        if colour == FACTOR:
            block = self.factors.at[self.core, rnd, coordinate("z"), coordinate("y"), coordinate("x"), rows, :]
            send(block, SEMS[rnd, colour, phase, kind, None])
        elif "z" in whole:
            for plane in reversed(range(SIDE)) if planes is None else planes:
                panels(plane, SEMS[rnd, colour, phase, kind, plane])
        else:
            plane_here = self.shifted("z", source) if axis == "z" else self.me["z"]
            for plane in range(SIDE):
                pl.when(plane_here == plane)(
                    lambda plane=plane: panels(plane, SEMS[rnd, colour, phase, kind, None])
                )

    def start_own(self, rnd, colour, phase, planes=None):
        for kind in ("A+", "A-"):
            self.each(rnd, colour, phase, kind, 0, lambda copy: copy.start(), planes)

    def forward(self, rnd, colour, phase, planes=None):
        for kind, relay, source in (("A+", "F+", -1), ("A-", "F-", 1)):
            self.each(rnd, colour, phase, kind, source, lambda copy: copy.wait_recv(), planes)
            self.each(rnd, colour, phase, relay, source, lambda copy: copy.start(), planes)

    def finish(self, rnd, colour, phase, planes=None):
        for kind, source in (("F+", -2), ("F-", 2)):
            self.each(rnd, colour, phase, kind, source, lambda copy: copy.wait_recv(), planes)

    def event(self, name, rnd, colour, plane=None):
        planes = None if plane is None else (plane,)
        if name == "A1":
            self.start_own(rnd, colour, 0)
        elif name in ("F1", "F2", "F3"):
            self.forward(rnd, colour, int(name[1]) - 1, planes)
        elif name in ("A2", "A3"):
            phase = int(name[1]) - 1
            if planes is None or "z" in axes_of(rnd, colour)[: phase - 1]:
                self.finish(rnd, colour, phase - 1, planes)
            elif plane == SIDE - 1:
                self.finish(rnd, colour, phase - 1)
            self.start_own(rnd, colour, phase, planes)
        else:
            self.finish(rnd, colour, 2, planes)

    def drain(self):
        for rnd in range(ROUNDS):
            for colour in range(4):
                for phase in range(3):
                    for kind, source in (("A+", 0), ("A-", 0), ("F+", -1), ("F-", 1)):
                        self.each(rnd, colour, phase, kind, source, lambda copy: copy.wait_send())


LOW, MID, TOP = range(ROUNDS)
XYZ, YZX, ZXY = range(3)
Z0, Z1, Z2, Z3 = range(SIDE)
OPENING = (
    (
        ("A1", MID, ZXY), ("A1", TOP, YZX), ("A1", TOP, XYZ), ("A1", TOP, ZXY), ("A1", MID, XYZ), ("A1", MID, YZX),
        ("A1", LOW, ZXY), ("F1", TOP, XYZ), ("A1", LOW, XYZ), ("F1", TOP, YZX), ("F1", MID, ZXY),
    ),
    (
        ("F1", MID, XYZ), ("F1", TOP, ZXY), ("A2", TOP, YZX), ("A2", TOP, XYZ), ("F1", LOW, XYZ),
    ),
    (
        ("A2", MID, ZXY, Z3), ("A2", MID, ZXY, Z2), ("F1", LOW, ZXY), ("A2", TOP, ZXY, Z3), ("A2", TOP, ZXY, Z0),
        ("F1", MID, YZX), ("A2", TOP, ZXY, Z1), ("A2", MID, XYZ), ("A2", TOP, ZXY, Z2), ("F2", TOP, XYZ),
        ("F2", TOP, YZX), ("A2", MID, ZXY, Z1), ("A2", MID, YZX), ("F2", MID, ZXY, Z3), ("A2", LOW, ZXY, Z3),
    ),
    (
        ("A1", LOW, YZX), ("A3", TOP, YZX, Z3), ("A2", LOW, XYZ), ("A3", MID, ZXY, Z3), ("F2", TOP, ZXY, Z0),
        ("F2", TOP, ZXY, Z1),
    ),
    (
        ("F2", MID, XYZ), ("A2", MID, ZXY, Z0), ("F2", TOP, ZXY, Z3), ("A3", TOP, XYZ), ("F2", TOP, ZXY, Z2),
        ("A3", TOP, YZX, Z0), ("A2", LOW, ZXY, Z1), ("F2", MID, ZXY, Z1), ("A2", LOW, ZXY, Z0),
    ),
    (
        ("F2", LOW, ZXY, Z3), ("A3", TOP, ZXY, Z3), ("F3", TOP, YZX, Z0), ("F2", MID, ZXY, Z0), ("A3", TOP, YZX, Z1),
        ("A1", MID, FACTOR), ("F3", MID, ZXY, Z3), ("A1", TOP, FACTOR), ("F2", MID, YZX), ("A3", TOP, YZX, Z2),
        ("F1", TOP, FACTOR), ("F1", LOW, YZX), ("F1", MID, FACTOR), ("F3", TOP, ZXY, Z3), ("F3", TOP, XYZ),
        ("A3", TOP, ZXY, Z2), ("A3", TOP, ZXY, Z1), ("A3", LOW, ZXY, Z3), ("A1", LOW, FACTOR), ("A2", TOP, FACTOR),
        ("F2", MID, ZXY, Z2), ("A2", MID, FACTOR), ("A3", MID, YZX, Z3), ("A2", LOW, YZX), ("F3", TOP, YZX, Z3),
        ("F1", LOW, FACTOR), ("A3", TOP, ZXY, Z0), ("A2", LOW, ZXY, Z2), ("D", TOP, ZXY, Z3), ("F2", MID, FACTOR),
        ("D", TOP, YZX, Z0), ("D", TOP, XYZ), ("F2", TOP, FACTOR), ("D", TOP, YZX, Z3), ("F3", TOP, YZX, Z2),
        ("A3", MID, YZX, Z1), ("A3", TOP, FACTOR), ("D", MID, ZXY, Z3), ("A2", LOW, FACTOR), ("A3", MID, XYZ),
        ("F2", LOW, ZXY, Z0), ("F3", TOP, YZX, Z1), ("F3", TOP, ZXY, Z1), ("F3", MID, YZX, Z1), ("F3", TOP, FACTOR),
        ("F3", TOP, ZXY, Z0), ("F3", TOP, ZXY, Z2), ("F2", LOW, XYZ), ("F2", LOW, FACTOR), ("D", TOP, YZX, Z2),
        ("A3", MID, ZXY, Z2), ("F2", LOW, ZXY, Z2), ("A3", MID, FACTOR), ("D", TOP, FACTOR), ("D", TOP, ZXY, Z1),
    ),
)
BEFORE_STEP = {
    1: (
        ("F2", LOW, YZX), ("A3", MID, YZX, Z2), ("D", TOP, ZXY, Z2), ("F3", MID, FACTOR), ("A3", MID, ZXY, Z1),
        ("A3", MID, ZXY, Z0), ("D", TOP, YZX, Z1), ("A3", MID, YZX, Z0),
    ),
    4: (
        ("F3", MID, XYZ),
    ),
    5: (
        ("F3", MID, YZX, Z3), ("A3", LOW, FACTOR), ("A3", LOW, XYZ), ("D", TOP, ZXY, Z0), ("F3", MID, ZXY, Z2),
    ),
    6: (
        ("A3", LOW, ZXY, Z2), ("F3", MID, YZX, Z2), ("A3", LOW, YZX, Z3), ("D", MID, FACTOR), ("F3", MID, ZXY, Z1),
    ),
    8: (
        ("D", MID, YZX, Z3), ("A3", LOW, YZX, Z2), ("F3", MID, YZX, Z0), ("F3", LOW, ZXY, Z3), ("D", MID, YZX, Z2),
        ("D", MID, ZXY, Z2), ("D", MID, YZX, Z1), ("F3", MID, ZXY, Z0), ("F2", LOW, ZXY, Z1), ("D", MID, XYZ),
    ),
    11: (
        ("F3", LOW, YZX, Z3),
    ),
    12: (
        ("F3", LOW, FACTOR), ("D", MID, ZXY, Z1),
    ),
    13: (
        ("F3", LOW, ZXY, Z2), ("F3", LOW, YZX, Z2),
    ),
    14: (
        ("F3", LOW, XYZ), ("D", MID, ZXY, Z0), ("D", MID, YZX, Z0), ("A3", LOW, YZX, Z1), ("D", LOW, ZXY, Z3),
        ("A3", LOW, ZXY, Z1), ("A3", LOW, YZX, Z0), ("A3", LOW, ZXY, Z0),
    ),
    15: (
        ("D", LOW, FACTOR), ("D", LOW, ZXY, Z2), ("D", LOW, YZX, Z2),
    ),
    16: (
        ("D", LOW, YZX, Z3), ("D", LOW, XYZ),
    ),
    17: (
        ("F3", LOW, ZXY, Z1), ("F3", LOW, YZX, Z1),
    ),
    20: (
        ("F3", LOW, ZXY, Z0), ("D", LOW, ZXY, Z1), ("D", LOW, YZX, Z1), ("F3", LOW, YZX, Z0),
    ),
    22: (
        ("D", LOW, YZX, Z0), ("D", LOW, ZXY, Z0),
    ),
}


def nt(lhs, rhs):
    return lax.dot_general(lhs, rhs, (((1,), (1,)), ((), ())), precision=PRECISE, preferred_element_type=jnp.float32)


def nn(lhs, rhs):
    return lax.dot_general(lhs, rhs, (((1,), (0,)), ((), ())), precision=PRECISE, preferred_element_type=jnp.float32)


def merge_factor(t, gram):
    row = lax.broadcasted_iota(jnp.int32, (GROUP, GROUP), 0)
    column = lax.broadcasted_iota(jnp.int32, (GROUP, GROUP), 1)
    for width in (BLK, 2 * BLK, 4 * BLK):
        above = (row // (2 * width) == column // (2 * width)) & (row // width < column // width)
        upper, lower = (t.reshape(-1, 2, width, GROUP)[:, half].reshape(GROUP // 2, GROUP) for half in range(2))
        upper = upper - nn(nn(upper, jnp.where(above, gram, 0.0)), t)
        t = jnp.stack([half.reshape(-1, width, GROUP) for half in (upper, lower)], axis=1).reshape(GROUP, GROUP)
    return t


def kernel(
    z_ref, v_ref, octet_ref, t_ref, out_ref, buf, factors, acc, peer, t_buf, rows_buf, gram, gram_peer, gram_pair,
    gram_parts, gram_full,
    send_sems, recv_sems, own_sems, z_keep_sems, z_send_sems, z_recv_sems, peer_send, peer_recv, octet_send, octet_recv, pair_send, pair_recv,
):
    gather = Gather(buf, factors, send_sems, recv_sems)
    me, core = gather.me, gather.core
    col = lax.axis_index("col")
    partner = (gather.kpt, col, 1 - core)
    seat = col % OCTET
    mates = {hop: (seat + hop) % OCTET for hop in range(1, OCTET)}

    def mate(hop):
        return (gather.kpt, col - seat + mates[hop], core)

    def to_mate(stage, hop, source, target):
        sem = stage * OCTET + hop
        return pltpu.make_async_remote_copy(
            src_ref=source, dst_ref=target, send_sem=octet_send.at[sem], recv_sem=octet_recv.at[sem],
            device_id=mate(hop), device_id_type=MESH,
        )

    def to_partner(sem, source, target):
        return pltpu.make_async_remote_copy(
            src_ref=source, dst_ref=target, send_sem=pair_send.at[sem], recv_sem=pair_recv.at[sem],
            device_id=partner, device_id_type=MESH,
        )

    own = []
    for rnd in range(ROUNDS):
        chunks = pl.ds(ROUND_BASE[rnd], CHUNKS - OCTET * rnd)
        rows = pl.ds(ROWS_BASE[rnd], ROUNDS - rnd)
        to_buf = (v_ref.at[rnd, pl.ds(OCTET * rnd, CHUNKS - OCTET * rnd)], buf.at[chunks, me["z"], me["y"], me["x"]])
        to_rows = (octet_ref.at[rnd, pl.ds(rnd, ROUNDS - rnd), seat], rows_buf.at[rows, seat])
        own.append(pltpu.make_async_copy(*to_buf, own_sems.at[rnd]))
        own.append(pltpu.make_async_copy(*to_rows, own_sems.at[ROUNDS + rnd]))
    for rnd in range(ROUNDS):
        own.append(pltpu.make_async_copy(t_ref.at[8 * rnd + col // OCTET], t_buf.at[rnd], own_sems.at[2 * ROUNDS + rnd]))
    for copy in own:
        copy.start()
    mine = pl.ds(core * (COLS // 2), COLS // 2)

    def z_chunk(half, chunk):
        return z_ref.at[:, pl.ds(pl.multiple_of((half * CHUNKS + chunk) * LANES, LANES), LANES)]

    def z_keep(chunk):
        return pltpu.make_async_copy(z_chunk(core, chunk), out_ref.at[chunk, mine], z_keep_sems.at[chunk])

    def z_give(chunk):
        return pltpu.make_async_remote_copy(
            src_ref=z_chunk(1 - core, chunk), dst_ref=out_ref.at[chunk, mine],
            send_sem=z_send_sems.at[chunk], recv_sem=z_recv_sems.at[chunk],
            device_id=partner, device_id_type=MESH,
        )

    def each_chunk(action):
        def body(chunk, _):
            action(chunk)
            return 0

        lax.fori_loop(0, CHUNKS, body, 0)

    each_chunk(lambda chunk: z_keep(chunk).start())

    barrier = pltpu.get_barrier_semaphore()
    peers = [gather.neighbour(axis, offset) for axis in "xyz" for offset in (1, -1)]
    peers += [mate(hop) for hop in mates] + [partner]
    for device in peers:
        pl.semaphore_signal(barrier, inc=1, device_id=device, device_id_type=MESH)
    pl.semaphore_wait(barrier, len(peers))

    halves = [to_partner(2 + rnd, factors.at[core, rnd], factors.at[core, rnd]) for rnd in range(ROUNDS)]

    def run(events):
        for event in events:
            gather.event(*event)
            if event[0] == "D" and event[2] == FACTOR:
                halves[event[1]].start()

    spread = [
        to_mate(
            rnd, hop, octet_ref.at[rnd, pl.ds(rnd, ROUNDS - rnd), at], rows_buf.at[pl.ds(ROWS_BASE[rnd], ROUNDS - rnd), seat]
        )
        for rnd in range(ROUNDS) for hop, at in mates.items()
    ]
    for copy in spread:
        copy.start()
    for copy in own:
        copy.wait()
    run(OPENING[0])
    each_chunk(lambda chunk: z_give(chunk).start())
    for copy in spread:
        copy.wait()
    for rnd, chunks in enumerate(((0, 1, 2), (3, 4), (5,))):
        panel = jnp.concatenate([rows_buf[chunk].reshape(GROUP, LANES) for chunk in chunks], axis=1)
        gram[:, :, rnd] = nt(panel, panel).reshape(OCTET, 2, SHARE, GROUP)
    pair = to_partner(0, gram.at[:, 1 - core], gram_peer)
    pair.start()
    run(OPENING[1])
    pair.wait()
    gram_pair[...] = gram[:, core] + gram_peer[...]
    scatter = [to_mate(ROUNDS, hop, gram_pair.at[at], gram_parts.at[seat]) for hop, at in mates.items()]
    for copy in scatter:
        copy.start()
    gram_parts[seat] = gram_pair[seat]
    run(OPENING[2])
    for copy in scatter:
        copy.wait()
    gram_full[core, seat] = jnp.sum(gram_parts[...], axis=0)
    collect = [to_mate(ROUNDS + 1, hop, gram_full.at[core, seat], gram_full.at[core, seat]) for hop in mates]
    for copy in collect:
        copy.start()
    run(OPENING[3])
    for copy in collect:
        copy.wait()
    pair = to_partner(1, gram_full.at[core], gram_full.at[core])
    pair.start()
    run(OPENING[4])
    pair.wait()

    def merge(rnd, _):
        row = lax.broadcasted_iota(jnp.int32, (GROUP, GROUP), 0)
        column = lax.broadcasted_iota(jnp.int32, (GROUP, GROUP), 1)
        diagonal = jnp.where(row // BLK == column // BLK, jnp.concatenate([t_buf[rnd]] * OCTET, axis=1), 0.0)
        pieces = [gram_full[half, at, rnd] for at in range(OCTET) for half in range(2)]
        t_mat = merge_factor(diagonal, jnp.concatenate(pieces, axis=0)).T
        for half in range(2):
            rows_buf[2 * rnd + half] = t_mat[:, half * LANES : (half + 1) * LANES].reshape(OCTET, BLK, LANES)
        factors[core, rnd, me["z"], me["y"], me["x"]] = rows_buf[2 * rnd + core, seat]
        return 0

    lax.fori_loop(0, ROUNDS, merge, 0)
    run(OPENING[5])
    each_chunk(lambda chunk: z_keep(chunk).wait())
    each_chunk(lambda chunk: z_give(chunk).wait())

    def over_tiles(first, body):
        count = CHUNKS // 2 - first
        for size in (1, 2):
            pl.when(count // size % 2 == 1)(lambda size=size: body(first + count % size, size))
        for fours in (1, 2, 3):
            pl.when(count // 4 == fours)(lambda fours=fours: body(first + count % 4, 4 * fours))

    def step(idx, _):
        for at, events in BEFORE_STEP.items():
            @pl.when(idx == at)
            def _(events=events):
                run(events)

        for needed in range(ROUNDS):
            pl.when(idx == 16 - 8 * needed)(lambda needed=needed: halves[needed].wait())

        group = STEPS - 1 - idx
        rnd = group // 8
        plane = (group % 8) // 2
        pair_row = (group % 2) * 2
        slot = idx % 2
        shift = 16 * rnd - 4 * rnd * (rnd - 1)
        first = 4 * rnd + plane

        def tile(w):
            halves = [
                buf[shift + 2 * w + half, plane, pl.ds(pair_row, 2), :, :, :].reshape(GROUP, LANES) for half in range(2)
            ]
            return jnp.concatenate(halves, axis=1)

        def z_tile(w):
            return jnp.concatenate([out_ref[2 * w], out_ref[2 * w + 1]], axis=1)

        acc[...] = jnp.zeros_like(acc)

        def project(w, count):
            z = jnp.concatenate([z_tile(w + i) for i in range(count)], axis=1)
            acc[...] += nt(z, jnp.concatenate([tile(w + i) for i in range(count)], axis=1))

        over_tiles(first, project)

        exchange = pltpu.make_async_remote_copy(
            src_ref=acc, dst_ref=peer.at[slot], send_sem=peer_send.at[slot], recv_sem=peer_recv.at[slot],
            device_id=partner, device_id_type=MESH,
        )
        exchange.start()

        t_mat = jnp.concatenate(
            [factors[half, rnd, plane, pl.ds(pair_row, 2)].reshape(GROUP, LANES) for half in range(2)], axis=1
        )
        exchange.wait()
        w_full = nn(acc[...] + peer[slot], t_mat)

        def update(w, count):
            delta = nn(w_full, jnp.concatenate([tile(w + i) for i in range(count)], axis=1))
            for i in range(2 * count):
                out_ref[2 * w + i] -= delta[:, i * LANES : (i + 1) * LANES]

        over_tiles(first, update)
        return 0

    lax.fori_loop(0, STEPS, step, 0)
    gather.drain()


def apply_panels(z, v, t):
    def vmem(*shape):
        return pltpu.VMEM(shape, jnp.float32)

    return pl.pallas_call(
        kernel,
        out_shape=jax.ShapeDtypeStruct((CHUNKS, COLS, LANES), jnp.float32),
        in_specs=[pl.BlockSpec(memory_space=pl.ANY)] * 4,
        out_specs=pl.BlockSpec(memory_space=pltpu.VMEM),
        scratch_shapes=[
            vmem(SLOTS, SIDE, SIDE, SIDE, BLK, LANES),
            vmem(2, ROUNDS, SIDE, SIDE, SIDE, BLK, LANES),
            vmem(COLS, GROUP),
            vmem(2, COLS, GROUP),
            vmem(ROUNDS, GROUP, BLK),
            vmem(SLOTS // OCTET, OCTET, BLK, LANES),
            vmem(OCTET, 2, ROUNDS, SHARE, GROUP),
            vmem(OCTET, ROUNDS, SHARE, GROUP),
            vmem(OCTET, ROUNDS, SHARE, GROUP),
            vmem(OCTET, ROUNDS, SHARE, GROUP),
            vmem(2, OCTET, ROUNDS, SHARE, GROUP),
            pltpu.SemaphoreType.DMA((len(SEMS),)),
            pltpu.SemaphoreType.DMA((len(SEMS),)),
            pltpu.SemaphoreType.DMA((3 * ROUNDS,)),
            pltpu.SemaphoreType.DMA((CHUNKS,)),
            pltpu.SemaphoreType.DMA((CHUNKS,)),
            pltpu.SemaphoreType.DMA((CHUNKS,)),
            pltpu.SemaphoreType.DMA((2,)),
            pltpu.SemaphoreType.DMA((2,)),
            pltpu.SemaphoreType.DMA(((ROUNDS + 2) * OCTET,)),
            pltpu.SemaphoreType.DMA(((ROUNDS + 2) * OCTET,)),
            pltpu.SemaphoreType.DMA((2 + ROUNDS,)),
            pltpu.SemaphoreType.DMA((2 + ROUNDS,)),
        ],
        compiler_params=pltpu.CompilerParams(collective_id=0, has_side_effects=True, vmem_limit_bytes=67043328),
        name="apply_panels",
    )(z, v, v.reshape(ROUNDS, CHUNKS // OCTET, OCTET, BLK, LANES), t)


def solution(mesh):
    def local_run(z_cols, v_local, t_local):
        z = z_cols.T
        v = v_local.reshape(CHUNKS, LANES, ROUNDS, BLK).transpose(2, 0, 3, 1)
        out = apply_panels(z, v, t_local.reshape(STEPS, GROUP, BLK))
        return out.transpose(0, 2, 1).reshape(CHUNKS * LANES, COLS)

    return jax.shard_map(
        local_run,
        mesh=mesh,
        in_specs=(P("kpt", ("col", "row")), P(("kpt", "row"), "col"), P("kpt", None, None)),
        out_specs=P(("kpt", "row"), "col"),
        check_vma=False,
    )
```

```python
import jax
import jax.numpy as jnp
from jax import lax
from jax.experimental import pallas as pl
from jax.experimental.pallas import tpu as pltpu
from jax.sharding import PartitionSpec as P

PRECISE = lax.Precision.HIGHEST
MESH = pl.DeviceIdType.MESH

SIDE = 4
BLK = 32
ROUNDS = 3
LANES = 128
CHUNKS = 24
GROUP = 256
STEPS = 24
COLS = 64

ORDER = (("x", "y", "z"), ("y", "z", "x"), ("z", "x", "y"))
SHARES = {
    24: (4, 10, 10), 22: (4, 9, 9), 20: (4, 8, 8), 18: (4, 7, 7),
    16: (4, 6, 6), 14: (4, 5, 5), 12: (4, 4, 4), 10: (4, 3, 3),
    8: (2, 3, 3), 6: (2, 2, 2), 4: (2, 1, 1), 2: (1, 1, 0),
}
ROWS_BASE = (0, 3, 5)
ROUND_BASE = (0, 24, 40)
SLOTS = 48
KINDS = ("A+", "A-", "F+", "F-")
FACTOR = 3
OCTET = 8
SHARE = 16


def axes_of(rnd, colour):
    return ORDER[rnd if colour == FACTOR else colour]


def part(rnd, z_src, colour):
    first = 8 * rnd + 2 * z_src
    shares = SHARES[CHUNKS - first]
    return ROUND_BASE[rnd] + first - 8 * rnd + sum(shares[:colour]), shares[colour]


def sem_table():
    table = {}
    for rnd in range(ROUNDS):
        for colour in range(4):
            for phase in range(3):
                planes = range(SIDE) if colour != FACTOR and "z" in ORDER[colour][:phase] else (None,)
                for kind in KINDS:
                    for plane in planes:
                        table[rnd, colour, phase, kind, plane] = len(table)
    return table


SEMS = sem_table()


class Gather:
    def __init__(self, buf, factors, send_sems, recv_sems):
        col = lax.axis_index("col")
        self.kpt, self.core = lax.axis_index("kpt"), lax.axis_index("row")
        self.me = {"z": col // 16, "y": (col // 4) % 4, "x": col % 4}
        self.buf, self.factors, self.send_sems, self.recv_sems = buf, factors, send_sems, recv_sems
        self.at = {(axis, offset): (self.me[axis] + offset) % SIDE for axis in "xyz" for offset in (1, 2, 3)}
        self.peer = {(axis, offset): self.find(axis, offset) for axis in "xyz" for offset in (1, 3)}

    def find(self, axis, offset):
        at = dict(self.me)
        at[axis] = self.at[axis, offset]
        return (self.kpt, at["z"] * 16 + at["y"] * 4 + at["x"], self.core)

    def shifted(self, axis, offset):
        return self.me[axis] if offset == 0 else self.at[axis, offset % SIDE]

    def neighbour(self, axis, offset):
        return self.peer[axis, offset % SIDE]

    def each(self, rnd, colour, phase, kind, source, fn, planes=None):
        axis = axes_of(rnd, colour)[phase]
        whole = axes_of(rnd, colour)[:phase]
        rows = {"A+": pl.ds(0, BLK), "A-": pl.ds(0, BLK), "F+": pl.ds(0, BLK // 2), "F-": pl.ds(BLK // 2, BLK // 2)}[kind]
        target = self.neighbour(axis, 1 if kind[1] == "+" else -1)

        def coordinate(name):
            if name in whole:
                return slice(None)
            return self.shifted(name, source) if name == axis else self.me[name]

        def send(block, sem):
            fn(
                pltpu.make_async_remote_copy(
                    src_ref=block, dst_ref=block,
                    send_sem=self.send_sems.at[sem], recv_sem=self.recv_sems.at[sem],
                    device_id=target, device_id_type=MESH,
                )
            )

        def panels(plane, sem):
            slot, count = part(rnd, plane, colour)
            if count:
                send(self.buf.at[pl.ds(slot, count), plane, coordinate("y"), coordinate("x"), rows, :], sem)

        if colour == FACTOR:
            block = self.factors.at[self.core, rnd, coordinate("z"), coordinate("y"), coordinate("x"), rows, :]
            send(block, SEMS[rnd, colour, phase, kind, None])
        elif "z" in whole:
            for plane in reversed(range(SIDE)) if planes is None else planes:
                panels(plane, SEMS[rnd, colour, phase, kind, plane])
        else:
            plane_here = self.shifted("z", source) if axis == "z" else self.me["z"]
            for plane in range(SIDE):
                pl.when(plane_here == plane)(
                    lambda plane=plane: panels(plane, SEMS[rnd, colour, phase, kind, None])
                )

    def start_own(self, rnd, colour, phase, planes=None):
        for kind in ("A+", "A-"):
            self.each(rnd, colour, phase, kind, 0, lambda copy: copy.start(), planes)

    def forward(self, rnd, colour, phase, planes=None):
        for kind, relay, source in (("A+", "F+", -1), ("A-", "F-", 1)):
            self.each(rnd, colour, phase, kind, source, lambda copy: copy.wait_recv(), planes)
            self.each(rnd, colour, phase, relay, source, lambda copy: copy.start(), planes)

    def finish(self, rnd, colour, phase, planes=None):
        for kind, source in (("F+", -2), ("F-", 2)):
            self.each(rnd, colour, phase, kind, source, lambda copy: copy.wait_recv(), planes)

    def event(self, name, rnd, colour, plane=None):
        planes = None if plane is None else (plane,)
        if name == "A1":
            self.start_own(rnd, colour, 0)
        elif name in ("F1", "F2", "F3"):
            self.forward(rnd, colour, int(name[1]) - 1, planes)
        elif name in ("A2", "A3"):
            phase = int(name[1]) - 1
            if planes is None or "z" in axes_of(rnd, colour)[: phase - 1]:
                self.finish(rnd, colour, phase - 1, planes)
            elif plane == SIDE - 1:
                self.finish(rnd, colour, phase - 1)
            self.start_own(rnd, colour, phase, planes)
        else:
            self.finish(rnd, colour, 2, planes)

    def drain(self):
        for rnd in range(ROUNDS):
            for colour in range(4):
                for phase in range(3):
                    for kind, source in (("A+", 0), ("A-", 0), ("F+", -1), ("F-", 1)):
                        self.each(rnd, colour, phase, kind, source, lambda copy: copy.wait_send())


LOW, MID, TOP = range(ROUNDS)
XYZ, YZX, ZXY = range(3)
Z0, Z1, Z2, Z3 = range(SIDE)
OPENING = (
    (
        ("A1", TOP, ZXY), ("A1", TOP, YZX), ("A1", LOW, ZXY), ("A1", MID, YZX), ("A1", TOP, XYZ), ("A1", LOW, XYZ),
        ("F1", TOP, ZXY), ("A1", MID, XYZ), ("A1", MID, ZXY), ("F1", TOP, YZX), ("F1", TOP, XYZ),
    ),
    (
        ("F1", LOW, ZXY), ("F1", MID, YZX), ("A2", TOP, ZXY, Z3), ("A2", TOP, ZXY, Z1), ("A2", TOP, XYZ),
        ("A2", TOP, ZXY, Z0), ("A2", TOP, ZXY, Z2), ("A2", TOP, YZX), ("F1", MID, ZXY), ("F1", MID, XYZ),
        ("A2", LOW, ZXY, Z3),
    ),
    (
        ("A1", LOW, YZX), ("F2", TOP, ZXY, Z3), ("A2", LOW, ZXY, Z0), ("F2", TOP, YZX),
    ),
    (
        ("A2", MID, YZX), ("F1", LOW, XYZ), ("F2", TOP, XYZ), ("A2", MID, XYZ), ("A2", MID, ZXY, Z3),
        ("F1", LOW, YZX), ("F2", LOW, ZXY, Z3), ("A3", TOP, YZX, Z3), ("F2", LOW, ZXY, Z0), ("A3", TOP, XYZ),
        ("A3", TOP, ZXY, Z3),
    ),
    (
        ("A3", TOP, YZX, Z1), ("A2", MID, ZXY, Z1), ("F2", TOP, ZXY, Z1), ("A2", LOW, ZXY, Z2), ("A3", LOW, ZXY, Z3),
        ("F2", TOP, ZXY, Z2),
    ),
    (
        ("A1", LOW, FACTOR), ("A1", MID, FACTOR), ("A2", LOW, XYZ), ("A3", TOP, YZX, Z0), ("A3", TOP, ZXY, Z2),
        ("F3", TOP, YZX, Z3), ("F1", LOW, FACTOR), ("F2", MID, YZX), ("A3", TOP, YZX, Z2), ("F2", MID, ZXY, Z3),
        ("F1", MID, FACTOR), ("A1", TOP, FACTOR), ("F2", TOP, ZXY, Z0), ("A2", MID, ZXY, Z0), ("A2", MID, ZXY, Z2),
        ("F2", MID, XYZ), ("F3", TOP, YZX, Z1), ("F3", TOP, XYZ), ("F2", LOW, ZXY, Z2), ("F1", TOP, FACTOR),
        ("A2", MID, FACTOR), ("F3", TOP, YZX, Z2), ("F2", MID, ZXY, Z0), ("F3", TOP, ZXY, Z2), ("A2", LOW, YZX),
        ("A3", TOP, ZXY, Z1), ("F2", MID, ZXY, Z1), ("A3", TOP, ZXY, Z0), ("A2", TOP, FACTOR), ("A3", MID, YZX, Z3),
        ("F2", TOP, FACTOR), ("F2", MID, ZXY, Z2), ("A3", MID, ZXY, Z3), ("F2", MID, FACTOR), ("A3", MID, YZX, Z2),
        ("A3", TOP, FACTOR), ("F3", TOP, ZXY, Z3), ("A3", MID, XYZ), ("F3", TOP, ZXY, Z1), ("A3", MID, YZX, Z0),
        ("F3", TOP, ZXY, Z0), ("F3", TOP, FACTOR), ("A2", LOW, FACTOR), ("A3", MID, FACTOR), ("A3", MID, ZXY, Z1),
        ("D", TOP, XYZ), ("F3", MID, YZX, Z0), ("D", TOP, YZX, Z1), ("D", TOP, YZX, Z3), ("A3", MID, ZXY, Z2),
        ("D", TOP, ZXY, Z3), ("D", TOP, FACTOR), ("F2", LOW, YZX), ("F3", LOW, ZXY, Z3), ("F2", LOW, FACTOR),
        ("D", TOP, ZXY, Z2), ("F3", MID, YZX, Z3),
    ),
)
BEFORE_STEP = {
    1: (
        ("F2", LOW, XYZ), ("F3", MID, YZX, Z2), ("D", TOP, ZXY, Z0), ("F3", TOP, YZX, Z0), ("D", TOP, YZX, Z2),
        ("F3", MID, FACTOR),
    ),
    2: (
        ("A2", LOW, ZXY, Z1),
    ),
    4: (
        ("F3", MID, ZXY, Z3), ("D", TOP, ZXY, Z1),
    ),
    5: (
        ("D", MID, YZX, Z2), ("F3", MID, ZXY, Z2), ("F3", MID, XYZ), ("F3", MID, ZXY, Z1), ("D", MID, FACTOR),
        ("A3", MID, ZXY, Z0), ("D", MID, YZX, Z0), ("A3", MID, YZX, Z1), ("D", MID, YZX, Z3),
    ),
    6: (
        ("A3", LOW, ZXY, Z2), ("F2", LOW, ZXY, Z1), ("D", TOP, YZX, Z0),
    ),
    7: (
        ("A3", LOW, YZX, Z3), ("A3", LOW, FACTOR), ("D", MID, ZXY, Z2),
    ),
    8: (
        ("A3", LOW, XYZ), ("F3", MID, YZX, Z1), ("D", MID, ZXY, Z3), ("A3", LOW, YZX, Z2), ("D", MID, XYZ),
    ),
    10: (
        ("D", MID, ZXY, Z1),
    ),
    11: (
        ("F3", MID, ZXY, Z0), ("A3", LOW, YZX, Z1), ("F3", LOW, YZX, Z3),
    ),
    12: (
        ("A3", LOW, ZXY, Z1), ("D", MID, YZX, Z1),
    ),
    13: (
        ("F3", LOW, FACTOR),
    ),
    14: (
        ("F3", LOW, XYZ), ("D", LOW, ZXY, Z3), ("F3", LOW, YZX, Z2), ("F3", LOW, ZXY, Z2), ("D", MID, ZXY, Z0),
    ),
    15: (
        ("D", LOW, FACTOR),
    ),
    16: (
        ("F3", LOW, ZXY, Z1), ("A3", LOW, ZXY, Z0), ("D", LOW, ZXY, Z2), ("F3", LOW, YZX, Z1), ("A3", LOW, YZX, Z0),
        ("D", LOW, YZX, Z3), ("D", LOW, XYZ),
    ),
    17: (
        ("D", LOW, YZX, Z2),
    ),
    19: (
        ("D", LOW, ZXY, Z1), ("D", LOW, YZX, Z1),
    ),
    20: (
        ("F3", LOW, ZXY, Z0), ("F3", LOW, YZX, Z0),
    ),
    22: (
        ("D", LOW, ZXY, Z0), ("D", LOW, YZX, Z0),
    ),
}


def nt(lhs, rhs):
    return lax.dot_general(lhs, rhs, (((1,), (1,)), ((), ())), precision=PRECISE, preferred_element_type=jnp.float32)


def nn(lhs, rhs):
    return lax.dot_general(lhs, rhs, (((1,), (0,)), ((), ())), precision=PRECISE, preferred_element_type=jnp.float32)


def merge_factor(t, gram):
    row = lax.broadcasted_iota(jnp.int32, (GROUP, GROUP), 0)
    column = lax.broadcasted_iota(jnp.int32, (GROUP, GROUP), 1)
    for width in (BLK, 2 * BLK, 4 * BLK):
        above = (row // (2 * width) == column // (2 * width)) & (row // width < column // width)
        upper, lower = (t.reshape(-1, 2, width, GROUP)[:, half].reshape(GROUP // 2, GROUP) for half in range(2))
        upper = upper - nn(nn(upper, jnp.where(above, gram, 0.0)), t)
        t = jnp.stack([half.reshape(-1, width, GROUP) for half in (upper, lower)], axis=1).reshape(GROUP, GROUP)
    return t


def kernel(
    z_ref, v_ref, octet_ref, t_ref, out_ref, buf, factors, acc, peer, t_buf, rows_buf, gram, gram_peer, gram_pair,
    gram_parts, gram_full,
    send_sems, recv_sems, own_sems, z_keep_sems, z_send_sems, z_recv_sems, peer_send, peer_recv, octet_send, octet_recv, pair_send, pair_recv,
):
    gather = Gather(buf, factors, send_sems, recv_sems)
    me, core = gather.me, gather.core
    col = lax.axis_index("col")
    partner = (gather.kpt, col, 1 - core)
    seat = col % OCTET
    mates = {hop: (seat + hop) % OCTET for hop in range(1, OCTET)}

    def mate(hop):
        return (gather.kpt, col - seat + mates[hop], core)

    def to_mate(stage, hop, source, target):
        sem = stage * OCTET + hop
        return pltpu.make_async_remote_copy(
            src_ref=source, dst_ref=target, send_sem=octet_send.at[sem], recv_sem=octet_recv.at[sem],
            device_id=mate(hop), device_id_type=MESH,
        )

    def to_partner(sem, source, target):
        return pltpu.make_async_remote_copy(
            src_ref=source, dst_ref=target, send_sem=pair_send.at[sem], recv_sem=pair_recv.at[sem],
            device_id=partner, device_id_type=MESH,
        )

    own = []
    for rnd in range(ROUNDS):
        chunks = pl.ds(ROUND_BASE[rnd], CHUNKS - OCTET * rnd)
        rows = pl.ds(ROWS_BASE[rnd], ROUNDS - rnd)
        to_buf = (v_ref.at[rnd, pl.ds(OCTET * rnd, CHUNKS - OCTET * rnd)], buf.at[chunks, me["z"], me["y"], me["x"]])
        to_rows = (octet_ref.at[rnd, pl.ds(rnd, ROUNDS - rnd), seat], rows_buf.at[rows, seat])
        own.append(pltpu.make_async_copy(*to_buf, own_sems.at[rnd]))
        own.append(pltpu.make_async_copy(*to_rows, own_sems.at[ROUNDS + rnd]))
    for rnd in range(ROUNDS):
        own.append(pltpu.make_async_copy(t_ref.at[8 * rnd + col // OCTET], t_buf.at[rnd], own_sems.at[2 * ROUNDS + rnd]))
    for copy in own:
        copy.start()
    mine = pl.ds(core * (COLS // 2), COLS // 2)

    def z_chunk(half, chunk):
        return z_ref.at[:, pl.ds(pl.multiple_of((half * CHUNKS + chunk) * LANES, LANES), LANES)]

    def z_keep(chunk):
        return pltpu.make_async_copy(z_chunk(core, chunk), out_ref.at[chunk, mine], z_keep_sems.at[chunk])

    def z_give(chunk):
        return pltpu.make_async_remote_copy(
            src_ref=z_chunk(1 - core, chunk), dst_ref=out_ref.at[chunk, mine],
            send_sem=z_send_sems.at[chunk], recv_sem=z_recv_sems.at[chunk],
            device_id=partner, device_id_type=MESH,
        )

    def each_chunk(action):
        def body(chunk, _):
            action(chunk)
            return 0

        lax.fori_loop(0, CHUNKS, body, 0)

    each_chunk(lambda chunk: z_keep(chunk).start())

    barrier = pltpu.get_barrier_semaphore()
    peers = [gather.neighbour(axis, offset) for axis in "xyz" for offset in (1, -1)]
    peers += [mate(hop) for hop in mates] + [partner]
    for device in peers:
        pl.semaphore_signal(barrier, inc=1, device_id=device, device_id_type=MESH)
    pl.semaphore_wait(barrier, len(peers))

    halves = [to_partner(2 + rnd, factors.at[core, rnd], factors.at[core, rnd]) for rnd in range(ROUNDS)]

    def run(events):
        for event in events:
            gather.event(*event)
            if event[0] == "D" and event[2] == FACTOR:
                halves[event[1]].start()

    spread = [
        to_mate(
            rnd, hop, octet_ref.at[rnd, pl.ds(rnd, ROUNDS - rnd), at], rows_buf.at[pl.ds(ROWS_BASE[rnd], ROUNDS - rnd), seat]
        )
        for rnd in range(ROUNDS) for hop, at in mates.items()
    ]
    for copy in spread:
        copy.start()
    for copy in own:
        copy.wait()
    run(OPENING[0])
    each_chunk(lambda chunk: z_give(chunk).start())
    for copy in spread:
        copy.wait()
    for rnd, chunks in enumerate(((0, 1, 2), (3, 4), (5,))):
        panel = jnp.concatenate([rows_buf[chunk].reshape(GROUP, LANES) for chunk in chunks], axis=1)
        gram[:, :, rnd] = nt(panel, panel).reshape(OCTET, 2, SHARE, GROUP)
    pair = to_partner(0, gram.at[:, 1 - core], gram_peer)
    pair.start()
    run(OPENING[1])
    pair.wait()
    gram_pair[...] = gram[:, core] + gram_peer[...]
    scatter = [to_mate(ROUNDS, hop, gram_pair.at[at], gram_parts.at[seat]) for hop, at in mates.items()]
    for copy in scatter:
        copy.start()
    gram_parts[seat] = gram_pair[seat]
    run(OPENING[2])
    for copy in scatter:
        copy.wait()
    gram_full[core, seat] = jnp.sum(gram_parts[...], axis=0)
    collect = [to_mate(ROUNDS + 1, hop, gram_full.at[core, seat], gram_full.at[core, seat]) for hop in mates]
    for copy in collect:
        copy.start()
    run(OPENING[3])
    for copy in collect:
        copy.wait()
    pair = to_partner(1, gram_full.at[core], gram_full.at[core])
    pair.start()
    run(OPENING[4])
    pair.wait()

    def merge(rnd, _):
        row = lax.broadcasted_iota(jnp.int32, (GROUP, GROUP), 0)
        column = lax.broadcasted_iota(jnp.int32, (GROUP, GROUP), 1)
        diagonal = jnp.where(row // BLK == column // BLK, jnp.concatenate([t_buf[rnd]] * OCTET, axis=1), 0.0)
        pieces = [gram_full[half, at, rnd] for at in range(OCTET) for half in range(2)]
        t_mat = merge_factor(diagonal, jnp.concatenate(pieces, axis=0)).T
        for half in range(2):
            rows_buf[2 * rnd + half] = t_mat[:, half * LANES : (half + 1) * LANES].reshape(OCTET, BLK, LANES)
        factors[core, rnd, me["z"], me["y"], me["x"]] = rows_buf[2 * rnd + core, seat]
        return 0

    lax.fori_loop(0, ROUNDS, merge, 0)
    run(OPENING[5])
    each_chunk(lambda chunk: z_keep(chunk).wait())
    each_chunk(lambda chunk: z_give(chunk).wait())

    def over_tiles(first, body):
        count = CHUNKS // 2 - first
        for size in (1, 2):
            pl.when(count // size % 2 == 1)(lambda size=size: body(first + count % size, size))
        for fours in (1, 2, 3):
            pl.when(count // 4 == fours)(lambda fours=fours: body(first + count % 4, 4 * fours))

    def step(idx, _):
        for at, events in BEFORE_STEP.items():
            @pl.when(idx == at)
            def _(events=events):
                run(events)

        for needed in range(ROUNDS):
            pl.when(idx == 16 - 8 * needed)(lambda needed=needed: halves[needed].wait())

        group = STEPS - 1 - idx
        rnd = group // 8
        plane = (group % 8) // 2
        pair_row = (group % 2) * 2
        slot = idx % 2
        shift = 16 * rnd - 4 * rnd * (rnd - 1)
        first = 4 * rnd + plane

        def tile(w):
            halves = [
                buf[shift + 2 * w + half, plane, pl.ds(pair_row, 2), :, :, :].reshape(GROUP, LANES) for half in range(2)
            ]
            return jnp.concatenate(halves, axis=1)

        def z_tile(w):
            return jnp.concatenate([out_ref[2 * w], out_ref[2 * w + 1]], axis=1)

        acc[...] = jnp.zeros_like(acc)

        def project(w, count):
            z = jnp.concatenate([z_tile(w + i) for i in range(count)], axis=1)
            acc[...] += nt(z, jnp.concatenate([tile(w + i) for i in range(count)], axis=1))

        over_tiles(first, project)

        exchange = pltpu.make_async_remote_copy(
            src_ref=acc, dst_ref=peer.at[slot], send_sem=peer_send.at[slot], recv_sem=peer_recv.at[slot],
            device_id=partner, device_id_type=MESH,
        )
        exchange.start()

        t_mat = jnp.concatenate(
            [factors[half, rnd, plane, pl.ds(pair_row, 2)].reshape(GROUP, LANES) for half in range(2)], axis=1
        )
        exchange.wait()
        w_full = nn(acc[...] + peer[slot], t_mat)

        def update(w, count):
            delta = nn(w_full, jnp.concatenate([tile(w + i) for i in range(count)], axis=1))
            for i in range(2 * count):
                out_ref[2 * w + i] -= delta[:, i * LANES : (i + 1) * LANES]

        over_tiles(first, update)
        return 0

    lax.fori_loop(0, STEPS, step, 0)
    gather.drain()


def apply_panels(z, v, t):
    def vmem(*shape):
        return pltpu.VMEM(shape, jnp.float32)

    return pl.pallas_call(
        kernel,
        out_shape=jax.ShapeDtypeStruct((CHUNKS, COLS, LANES), jnp.float32),
        in_specs=[pl.BlockSpec(memory_space=pl.ANY)] * 4,
        out_specs=pl.BlockSpec(memory_space=pltpu.VMEM),
        scratch_shapes=[
            vmem(SLOTS, SIDE, SIDE, SIDE, BLK, LANES),
            vmem(2, ROUNDS, SIDE, SIDE, SIDE, BLK, LANES),
            vmem(COLS, GROUP),
            vmem(2, COLS, GROUP),
            vmem(ROUNDS, GROUP, BLK),
            vmem(SLOTS // OCTET, OCTET, BLK, LANES),
            vmem(OCTET, 2, ROUNDS, SHARE, GROUP),
            vmem(OCTET, ROUNDS, SHARE, GROUP),
            vmem(OCTET, ROUNDS, SHARE, GROUP),
            vmem(OCTET, ROUNDS, SHARE, GROUP),
            vmem(2, OCTET, ROUNDS, SHARE, GROUP),
            pltpu.SemaphoreType.DMA((len(SEMS),)),
            pltpu.SemaphoreType.DMA((len(SEMS),)),
            pltpu.SemaphoreType.DMA((3 * ROUNDS,)),
            pltpu.SemaphoreType.DMA((CHUNKS,)),
            pltpu.SemaphoreType.DMA((CHUNKS,)),
            pltpu.SemaphoreType.DMA((CHUNKS,)),
            pltpu.SemaphoreType.DMA((2,)),
            pltpu.SemaphoreType.DMA((2,)),
            pltpu.SemaphoreType.DMA(((ROUNDS + 2) * OCTET,)),
            pltpu.SemaphoreType.DMA(((ROUNDS + 2) * OCTET,)),
            pltpu.SemaphoreType.DMA((2 + ROUNDS,)),
            pltpu.SemaphoreType.DMA((2 + ROUNDS,)),
        ],
        compiler_params=pltpu.CompilerParams(collective_id=0, has_side_effects=True, vmem_limit_bytes=67043328),
        name="apply_panels",
    )(z, v, v.reshape(ROUNDS, CHUNKS // OCTET, OCTET, BLK, LANES), t)


def solution(mesh):
    def local_run(z_cols, v_local, t_local):
        z = z_cols.T
        v = v_local.reshape(CHUNKS, LANES, ROUNDS, BLK).transpose(2, 0, 3, 1)
        out = apply_panels(z, v, t_local.reshape(STEPS, GROUP, BLK))
        return out.transpose(0, 2, 1).reshape(CHUNKS * LANES, COLS)

    return jax.shard_map(
        local_run,
        mesh=mesh,
        in_specs=(P("kpt", ("col", "row")), P(("kpt", "row"), "col"), P("kpt", None, None)),
        out_specs=P(("kpt", "row"), "col"),
        check_vma=False,
    )
```
